128 devices in a mesh: neg: 16 (over x, y), qry: 8 (over z, core).
Axes of the slice: x: 4, y: 4, z: 4, core: 2. Of those that a mesh axis runs over, the one named last changes fastest.
Arguments:
- items_table: bfloat16 [131072, 512], P('neg'), may hold values from -6 to 6
- fetch_rows: int32 [2048, 640], P(('neg', 'qry')), may hold values from 0 to 8191, as said below
- neighbour_slots: int32 [65536, 40], P(('neg', 'qry')), may hold values from 0 to 10239, as said below
- neighbour_count: int32 [65536], P(('neg', 'qry')), may hold values from 20 to 40
- self_slot: int32 [65536], P(('neg', 'qry')), may hold values from 0 to 10239
- negative_count: int32 [65536], P('neg'), may hold values from 1 to 999
- message_weight: bfloat16 [512, 512], replicated, may hold values from -0.25 to 0.25
- message_bias: float32 [512], replicated, may hold values from -3 to 3
- self_weight: bfloat16 [512, 512], replicated, may hold values from -0.25 to 0.25
- neighbour_weight: bfloat16 [512, 512], replicated, may hold values from -0.25 to 0.25
- output_bias: float32 [512], replicated, may hold values from -3 to 3
- queries: bfloat16 [8192, 512], P('qry'), may hold values from -8 to 8
Outputs:
- negative_embed: bfloat16 [65536, 512], P(('neg', 'qry'))
- query_lse: float32 [8192], P('qry')
The draws below stay inside these ranges and needn't reach their ends.
Inputs may be any that keep to these rules, and one draw needn't show every extreme that they name: Within one row of fetch_rows (one device's list for one partition) no item appears twice. `neighbour_slots`: every one of a device's 16 * 640 fetched rows is named by at least one live neighbour of that device's negatives.
All inputs are finite; a program needn't handle non-finite values.
Results may differ from the reference program's by a relative error of at most 0.0055.
Values may be sent and summed in bfloat16 or wider, within the bound.
A program may use at most 128 MiB of HBM per device.

```python
import math
import jax
import jax.numpy as jnp
from jax import lax

D = 512
K = 40
ITEM_DEV = 8192
NEG_DEV = 512
CAP = 640
NEG = 65536
QRY = 8192
ITEMS = 131072
N_NEG = 16
N_QRY = 8


def draw_queries(key, part):
    values = jnp.clip(jax.random.normal(key, (QRY, D), jnp.float32), -5.5, 5.5)
    return values.astype(jnp.bfloat16)


def draw_fetch_rows(key, part):
    row_keys = jax.random.split(jax.random.fold_in(key, 7), N_NEG * N_QRY * N_NEG)

    def one_row(row_key):
        return jax.random.permutation(row_key, ITEM_DEV)[:CAP].astype(jnp.int32)
    return jax.vmap(one_row)(row_keys).astype(jnp.int32)


def neighbour_draw(key):
    count_key = jax.random.fold_in(key, 11)
    counts = jax.random.randint(count_key, (NEG,), K // 2, K + 1, dtype=jnp.int32)
    slot_total = N_NEG * CAP
    device_keys = jax.random.split(jax.random.fold_in(key, 13), N_NEG * N_QRY)
    count_blocks = counts.reshape(N_NEG * N_QRY, NEG_DEV)

    def one_device(device_key, count_block):
        order_key = jax.random.fold_in(device_key, 1)
        filler_key = jax.random.fold_in(device_key, 2)
        live_mask = jnp.arange(K, dtype=jnp.int32)[None, :] < count_block[:, None]
        priority = jax.random.randint(order_key, (NEG_DEV * K,), 0, 1 << 20, dtype=jnp.int32)
        priority = priority + jnp.where(live_mask.reshape(-1), 0, 1 << 21).astype(jnp.int32)
        order = jnp.argsort(priority, stable=True).astype(jnp.int32)
        ranked = jnp.argsort(order, stable=True).astype(jnp.int32)
        filler = jax.random.randint(filler_key, (NEG_DEV * K,), 0, slot_total, dtype=jnp.int32)
        slots = jnp.where(ranked < slot_total, ranked, filler)
        return slots.reshape(NEG_DEV, K).astype(jnp.int32)
    slots = jax.vmap(one_device)(device_keys, count_blocks).reshape(NEG, K)
    return (counts, slots)


def draw_neighbour_count(key, part):
    return neighbour_draw(key)[0].astype(jnp.int32)


def draw_neighbour_slots(key, part):
    return neighbour_draw(key)[1].astype(jnp.int32)


def place_ends(drawn, stream_key, smallest, largest):
    longest = drawn.shape.index(max(drawn.shape))
    spots = []
    for shift in (0, 1):
        where = [jax.random.randint(jax.random.fold_in(stream_key, axis), (), 0, length) for axis, length in enumerate(drawn.shape)]
        where[longest] = (where[longest] + shift) % drawn.shape[longest]
        spots.append(tuple(where))
    return drawn.at[spots[0]].set(smallest).at[spots[1]].set(largest)


def shard_levels(own_key, shape, cuts, least, high):
    factor_of = 1.0
    for dim, parts in cuts:
        draws = jax.random.uniform(jax.random.fold_in(jax.random.fold_in(own_key, 6), dim), (parts,), jnp.float32, least / len(cuts), high / len(cuts))
        factor_of = factor_of * jnp.repeat(jnp.exp(draws), shape[dim] // parts).reshape((-1,) + (1,) * (len(shape) - 1 - dim))
    return factor_of


def gaussian(key, shape, deviation, limit, pieces=(), kind=jnp.bfloat16):
    factor_of = shard_levels(key, shape, pieces, -0.22, 0.18) if pieces else 1.0
    values = jax.random.normal(key, shape, jnp.float32) * deviation * factor_of
    return jnp.minimum(jnp.maximum(values, -limit), limit).astype(kind)


def setup_inputs(seed: int = 0) -> dict:
    seeds = jax.random.split(jax.random.key(seed), 13)
    items_table = gaussian(seeds[0], (ITEMS, D), 1.0, 6.0, ((0, 16),))
    fetch_rows = draw_fetch_rows(jax.random.fold_in(seeds[12], 71), 0)
    neighbour_slots = draw_neighbour_slots(jax.random.fold_in(seeds[12], 71), 0)
    neighbour_count = draw_neighbour_count(jax.random.fold_in(seeds[12], 71), 0)
    self_slot = place_ends(jax.random.randint(seeds[4], (NEG,), 0, N_NEG * CAP), jax.random.fold_in(seeds[4], 1), 0, (N_NEG * CAP) - 1).astype(jnp.int32)
    negative_count = place_ends(jax.random.randint(seeds[5], (NEG,), 1, 1000), jax.random.fold_in(seeds[5], 1), 1, 999).astype(jnp.int32)
    message_weight = gaussian(seeds[6], (D, D), D ** -0.5, 0.25)
    message_bias = gaussian(seeds[7], (D,), 0.5, 3.0, (), jnp.float32)
    self_weight = gaussian(seeds[8], (D, D), D ** -0.5, 0.25)
    neighbour_weight = gaussian(seeds[9], (D, D), D ** -0.5, 0.25)
    output_bias = gaussian(seeds[10], (D,), 0.5, 3.0, (), jnp.float32)
    queries = draw_queries(jax.random.fold_in(seeds[12], 71), 0)
    return {"items_table": items_table, "fetch_rows": fetch_rows, "neighbour_slots": neighbour_slots, "neighbour_count": neighbour_count, "self_slot": self_slot, "negative_count": negative_count, "message_weight": message_weight, "message_bias": message_bias, "self_weight": self_weight, "neighbour_weight": neighbour_weight, "output_bias": output_bias, "queries": queries}


def embed_device(items_table, fetch_block, slot_block, count_block, self_block, message_weight, message_bias, self_weight, neighbour_weight, output_bias):
    owners = jnp.arange(N_NEG, dtype=jnp.int32)[:, None] * ITEM_DEV
    global_rows = (fetch_block.astype(jnp.int32) + owners).reshape(-1)
    fetched = items_table[global_rows]
    message = jax.nn.relu(jnp.dot(fetched, message_weight, preferred_element_type=jnp.float32) + message_bias).astype(jnp.bfloat16)
    gathered = message[slot_block].astype(jnp.float32)
    live_mask = jnp.arange(K, dtype=jnp.int32)[None, :] < count_block[:, None]
    summed = lax.optimization_barrier(jnp.sum(jnp.where(live_mask[:, :, None], gathered, jnp.float32(0.0)), axis=1))
    neighbour_mean = (summed / count_block.astype(jnp.float32)[:, None]).astype(jnp.bfloat16)
    self_rows = fetched[self_block]
    hidden = jnp.dot(self_rows, self_weight, preferred_element_type=jnp.float32)
    hidden = hidden + jnp.dot(neighbour_mean, neighbour_weight, preferred_element_type=jnp.float32) + output_bias
    hidden = jax.nn.relu(hidden)
    scale_inv = lax.rsqrt(lax.optimization_barrier(jnp.mean(hidden * hidden, axis=-1, keepdims=True)) + 0.25)
    return (hidden * scale_inv).astype(jnp.bfloat16)

def reference(items_table, fetch_rows, neighbour_slots, neighbour_count, self_slot, negative_count, message_weight, message_bias, self_weight, neighbour_weight, output_bias, queries):
    devices_all = N_NEG * N_QRY
    fetch_all = fetch_rows.reshape(devices_all, N_NEG, -1)
    slots_all = neighbour_slots.reshape(devices_all, -1, K)
    counts_all = neighbour_count.reshape(devices_all, -1)
    selves_all = self_slot.reshape(devices_all, -1)

    def one_device(inputs):
        return embed_device(items_table, inputs[0], inputs[1], inputs[2], inputs[3], message_weight, message_bias, self_weight, neighbour_weight, output_bias)
    embedded = lax.map(one_device, (fetch_all, slots_all, counts_all, selves_all))
    negative_embed = embedded.reshape(-1, D)
    log_count = jnp.log(negative_count.astype(jnp.float32))
    query_blocks = queries.reshape(N_QRY, -1, D)

    def one_block(query_block):
        scores = 0.25 * jnp.dot(query_block, negative_embed.T, preferred_element_type=jnp.float32) - log_count[None, :]
        peak = lax.optimization_barrier(jnp.max(scores, axis=1))
        totals = lax.optimization_barrier(jnp.sum(jnp.exp(scores - peak[:, None]), axis=1))
        return peak + jnp.log(totals) - math.log(NEG)
    query_lse = lax.map(one_block, query_blocks).reshape(-1)
    return (negative_embed, query_lse)
```

```python
import functools
import math

import jax
import jax.numpy as jnp
from jax import lax
from jax.experimental import pallas as pl
from jax.experimental.pallas import tpu as pltpu
from jax.sharding import PartitionSpec as P

MESH = pl.DeviceIdType.MESH
VMEM = pl.BlockSpec(memory_space=pltpu.VMEM)


def greet(peers):
    barrier = pltpu.get_barrier_semaphore()
    for peer in peers:
        pl.semaphore_signal(barrier, inc=1, device_id=peer, device_id_type=MESH)
    pl.semaphore_wait(barrier, len(peers))


def remote(src, dst, send, recv, peer):
    return pltpu.make_async_remote_copy(
        src_ref=src, dst_ref=dst, send_sem=send, recv_sem=recv, device_id=peer, device_id_type=MESH
    )


def index_kernel(rows_ref, slots_ref, last_ref, rows_out, aux_out, aux_own, send_sem, recv_sem):
    me = lax.axis_index("neg")
    peers = [{"neg": lax.rem(me + d, 16)} for d in range(1, 16)]
    count = lax.shift_right_logical(last_ref[...], 16)
    for h in range(2):
        ks = lax.broadcasted_iota(jnp.int32, (20, 512), 0) + 20 * h
        half = jnp.where(ks < count, slots_ref[20 * h:20 * h + 20, :], 0xFFFF)
        if h == 0:
            low = half
        else:
            aux_own[0:20, :] = low | jnp.left_shift(half, 16)
    aux_own[20:24, :] = jnp.broadcast_to(last_ref[...], (4, 512))
    greet(peers)
    copies = []
    for d, peer in enumerate(peers):
        other = lax.rem(me + d + 1, 16)
        copies.append(remote(rows_ref.at[other], rows_out.at[me], send_sem.at[0, d], recv_sem.at[0, d], peer))
    for d, peer in enumerate(peers):
        copies.append(remote(aux_own, aux_out.at[me], send_sem.at[1, d], recv_sem.at[1, d], peer))
    for copy in copies:
        copy.start()
    rows_out[me] = rows_ref[me]
    aux_out[me] = aux_own[...]
    for copy in copies:
        copy.wait()


def exchange_indices(fetch_rows, slots, last):
    return pl.pallas_call(
        index_kernel,
        out_shape=(
            jax.ShapeDtypeStruct((16, 1, 640), jnp.int32),
            jax.ShapeDtypeStruct((16, 24, 512), jnp.int32),
        ),
        in_specs=[VMEM] * 3,
        out_specs=(VMEM, VMEM),
        scratch_shapes=[
            pltpu.VMEM((24, 512), jnp.int32),
            pltpu.SemaphoreType.DMA((2, 15)),
            pltpu.SemaphoreType.DMA((2, 15)),
        ],
        compiler_params=pltpu.CompilerParams(collective_id=1, has_side_effects=True),
        name="exchange_indices",
    )(fetch_rows, slots, last)


def partial_kernel(get_p, rows_ref, aux_ref, table_ref, wm_ref, ws_ref, wn_ref, bm_ref, out_ref,
                   t_ref, tbuf, g_ref, gb_ref, c_ref, key_ref, val_ref, self_ref, rcnt_ref, pbuf, in_sem, out_sem):
    p = get_p()
    blocks = 16
    blk = 512

    def fetch(i, slot):
        return pltpu.make_async_copy(table_ref.at[pl.ds(i * blk, blk), :], tbuf.at[slot], in_sem.at[slot])

    fetch(0, 0).start()

    def build(i, _):
        slot = lax.rem(i, 2)

        @pl.when(i + 1 < blocks)
        def _():
            fetch(i + 1, 1 - slot).start()
        fetch(i, slot).wait()
        x = tbuf[slot]
        m = jnp.dot(x, wm_ref[...], preferred_element_type=jnp.float32) + bm_ref[...]
        m = jnp.maximum(m, 0.0).astype(jnp.bfloat16)
        t1 = jnp.dot(m, wn_ref[...], preferred_element_type=jnp.float32)
        t2 = jnp.dot(x, ws_ref[...], preferred_element_type=jnp.float32)
        base = pl.multiple_of(i * (blk * 8), 8)
        for j in range(4):
            t_ref[pl.ds(base + j, blk, stride=8), :] = t1[:, j * 128:(j + 1) * 128]
            t_ref[pl.ds(base + 4 + j, blk, stride=8), :] = t2[:, j * 128:(j + 1) * 128]
        return 0
    lax.fori_loop(0, blocks, build, 0)

    last = aux_ref[:, 20, :]
    last = jnp.concatenate([last] * 8, axis=0)
    self_ref[...] = (last & 0xFFFF).T
    rcnt_ref[...] = (1.0 / (last >> 16).astype(jnp.float32)).T

    lane = lax.broadcasted_iota(jnp.int32, (128, 128), 1)
    sub = lax.broadcasted_iota(jnp.int32, (128, 128), 0)

    def one(n, _):
        slot = lax.rem(n, 2)

        def gather(i, _):
            for u in range(32):
                s = i * 32 + u
                r = rows_ref[n, s]
                g_ref[pl.ds(pl.multiple_of(s * 8, 8), 8), :] = t_ref[pl.ds(pl.multiple_of(r * 8, 8), 8), :]
            return 0
        lax.fori_loop(0, 20, gather, 0)
        for j in range(8):
            gb_ref[:, j * 128:(j + 1) * 128] = g_ref[pl.ds(j, 640, stride=8), :].astype(jnp.bfloat16)
        packed = aux_ref[n][:24]
        for h, slots in enumerate((packed & 0xFFFF, lax.shift_right_logical(packed, 16))):
            rel = slots - 640 * p
            ok = (rel >= 0) & (rel < 640)
            key_ref[h * 24:(h + 1) * 24, :] = rel & 127
            val_ref[h * 24:(h + 1) * 24, :] = jnp.where(ok, jnp.left_shift(1, 6 * (lax.shift_right_logical(rel, 7) & 7) & 31), 0)
        for vb in range(4):
            cols = pl.ds(vb * 128, 128)
            acc = jnp.zeros((128, 128), jnp.int32)
            for k in range(40):
                kk = k if k < 20 else k + 4
                key = jnp.broadcast_to(key_ref[kk:kk + 1, cols], (128, 128))
                val = jnp.broadcast_to(val_ref[kk:kk + 1, cols], (128, 128))
                acc = acc + jnp.where(sub == key, val, 0)
            ct = acc.T
            here = lane == n
            self_col = jnp.sum(jnp.where(here, self_ref[cols, :].astype(jnp.float32), 0.0), axis=1, keepdims=True).astype(jnp.int32) - 640 * p
            for f in range(5):
                c_ref[cols, f * 128:(f + 1) * 128] = (lax.shift_right_logical(ct, 6 * f) & 63).astype(jnp.float32).astype(jnp.bfloat16)
                c_ref[cols, 640 + f * 128:640 + (f + 1) * 128] = jnp.where(self_col == lane + f * 128, 1.0, 0.0).astype(jnp.bfloat16)
        here = lax.broadcasted_iota(jnp.int32, (512, 128), 1) == n
        rcnt = jnp.sum(jnp.where(here, rcnt_ref[...], 0.0), axis=1, keepdims=True)
        part = jnp.dot(c_ref[:, :640], gb_ref[:, :512], preferred_element_type=jnp.float32) * rcnt
        part = part + jnp.dot(c_ref[:, 640:], gb_ref[:, 512:], preferred_element_type=jnp.float32)

        def send(slot, n):
            return pltpu.make_async_copy(pbuf.at[slot], out_ref.at[n], out_sem.at[slot])

        @pl.when(n >= 2)
        def _():
            send(slot, n - 2).wait()
        pbuf[slot] = part.astype(jnp.bfloat16)
        send(slot, n).start()
        return 0
    lax.fori_loop(0, 16, one, 0)
    for slot in range(2):
        pltpu.make_async_copy(pbuf.at[slot], out_ref.at[14 + slot], out_sem.at[slot]).wait()


def partials(get_p, rows, aux, table, wm, ws, wn, bm):
    vmem = pl.BlockSpec(memory_space=pltpu.VMEM)
    return pl.pallas_call(
        functools.partial(partial_kernel, get_p),
        out_shape=jax.ShapeDtypeStruct((16, 512, 512), jnp.bfloat16),
        in_specs=[pl.BlockSpec(memory_space=pltpu.SMEM), vmem, pl.BlockSpec(memory_space=pl.ANY), vmem, vmem, vmem, vmem],
        out_specs=pl.BlockSpec(memory_space=pl.ANY),
        scratch_shapes=[
            pltpu.VMEM((65536, 128), jnp.float32),
            pltpu.VMEM((2, 512, 512), jnp.bfloat16),
            pltpu.VMEM((5120, 128), jnp.float32),
            pltpu.VMEM((640, 1024), jnp.bfloat16),
            pltpu.VMEM((512, 1280), jnp.bfloat16),
            pltpu.VMEM((48, 512), jnp.int32),
            pltpu.VMEM((48, 512), jnp.int32),
            pltpu.VMEM((512, 128), jnp.int32),
            pltpu.VMEM((512, 128), jnp.float32),
            pltpu.VMEM((2, 512, 512), jnp.bfloat16),
            pltpu.SemaphoreType.DMA((2,)),
            pltpu.SemaphoreType.DMA((2,)),
        ],
        compiler_params=pltpu.CompilerParams(vmem_limit_bytes=60 * 1024 * 1024),
        cost_estimate=pl.CostEstimate(flops=24_000_000_000, bytes_accessed=24_000_000, transcendentals=0),
        name="partials",
    )(rows, aux, table, wm, ws, wn, bm)


def reduce_kernel(p_ref, out_ref, near, far, carry, total, near2, far2, carry2, send_sem, recv_sem):
    me = lax.axis_index("neg")
    spot = (me // 4, lax.rem(me, 4))

    def device(axis, step):
        moved = lax.rem(spot[axis] + step + 4, 4)
        return {"neg": moved * 4 + spot[1] if axis == 0 else spot[0] * 4 + moved}

    greet([device(axis, step) for axis in range(2) for step in (1, -1)])
    base = (0, 256)

    def block(half, dest, lo, size):
        rows = pl.ds(base[half] + lo, size)
        return p_ref.at[dest, :, rows, :] if half == 0 else p_ref.at[:, dest, rows, :]

    first = {}
    for half in range(2):
        across = lax.rem(spot[half] + 2, 4)
        for w, step in enumerate((1, -1)):
            peer = device(half, step)
            first[half, w, 0] = remote(
                block(half, across, 128 * w, 128), near.at[half, w],
                send_sem.at[0, half, w, 0], recv_sem.at[0, half, w, 0], peer)
            dest = lax.rem(spot[half] + step + 4, 4)
            first[half, w, 1] = remote(
                block(half, dest, 128 * (1 - w), 128), far.at[half, w, 1],
                send_sem.at[0, half, w, 1], recv_sem.at[0, half, w, 1], peer)
            first[half, w, 2] = remote(
                carry.at[half, w], far.at[half, w, 0],
                send_sem.at[0, half, w, 2], recv_sem.at[0, half, w, 2], peer)
    for stage in range(2):
        for half in range(2):
            for w in range(2):
                first[half, w, stage].start()
    for half in range(2):
        for w, step in enumerate((1, -1)):
            first[half, w, 0].wait_recv()
            dest = lax.rem(spot[half] + step + 4, 4)
            for j in range(4):
                own = block(half, dest, 128 * w, 128)[j]
                carry[half, w, j] = (own.astype(jnp.float32) + near[half, w, j].astype(jnp.float32)).astype(jnp.bfloat16)
            first[half, w, 2].start()
    for half in range(2):
        for w in range(2):
            first[half, w, 1].wait_recv()
            first[half, w, 2].wait_recv()
        other = 1 - half
        home = spot[half]
        for j in range(4):
            for w in range(2):
                own = block(half, home, 128 * w, 128)[j]
                value = own.astype(jnp.float32) + far[half, w, 0, j].astype(jnp.float32)
                value = value + far[half, 1 - w, 1, j].astype(jnp.float32)
                total[half, j, w] = value
    second = {}
    for half in range(2):
        other = 1 - half
        across = lax.rem(spot[other] + 2, 4)
        for w, step in enumerate((1, -1)):
            peer = device(other, step)
            dest = lax.rem(spot[other] + step + 4, 4)
            carry2[half, w, 0] = total[half, across, w].astype(jnp.bfloat16)
            carry2[half, w, 1] = total[half, dest, 1 - w].astype(jnp.bfloat16)
            for stage, target in ((0, near2.at[half, w]), (1, far2.at[half, w, 1]), (2, far2.at[half, w, 0])):
                second[half, w, stage] = remote(
                    carry2.at[half, w, stage], target,
                    send_sem.at[1, half, w, stage], recv_sem.at[1, half, w, stage], peer)
            second[half, w, 0].start()
            second[half, w, 1].start()
    for half in range(2):
        other = 1 - half
        for w, step in enumerate((1, -1)):
            second[half, w, 0].wait_recv()
            dest = lax.rem(spot[other] + step + 4, 4)
            carry2[half, w, 2] = (total[half, dest, w] + near2[half, w].astype(jnp.float32)).astype(jnp.bfloat16)
            second[half, w, 2].start()
    for half in range(2):
        home = spot[1 - half]
        for w in range(2):
            second[half, w, 1].wait_recv()
            second[half, w, 2].wait_recv()
        for w in range(2):
            value = total[half, home, w] + far2[half, w, 0].astype(jnp.float32)
            value = value + far2[half, 1 - w, 1].astype(jnp.float32)
            out_ref[pl.ds(base[half] + 128 * w, 128), :] = value
    for copies in (first, second):
        for copy in copies.values():
            copy.wait_send()


def reduce_partials(partial):
    return pl.pallas_call(
        reduce_kernel,
        out_shape=jax.ShapeDtypeStruct((512, 512), jnp.float32),
        in_specs=[VMEM],
        out_specs=VMEM,
        scratch_shapes=[
            pltpu.VMEM((2, 2, 4, 128, 512), jnp.bfloat16),
            pltpu.VMEM((2, 2, 2, 4, 128, 512), jnp.bfloat16),
            pltpu.VMEM((2, 2, 4, 128, 512), jnp.bfloat16),
            pltpu.VMEM((2, 4, 2, 128, 512), jnp.float32),
            pltpu.VMEM((2, 2, 128, 512), jnp.bfloat16),
            pltpu.VMEM((2, 2, 2, 128, 512), jnp.bfloat16),
            pltpu.VMEM((2, 2, 3, 128, 512), jnp.bfloat16),
            pltpu.SemaphoreType.DMA((2, 2, 2, 3)),
            pltpu.SemaphoreType.DMA((2, 2, 2, 3)),
        ],
        compiler_params=pltpu.CompilerParams(
            collective_id=2, has_side_effects=True, vmem_limit_bytes=48 * 1024 * 1024),
        name="reduce_partials",
    )(partial.reshape(4, 4, 512, 512))


def score_kernel(pre_ref, bias_ref, logc_ref, queries_ref, embed_ref, stats_ref, scaled):
    @pl.when(pl.program_id(0) == 0)
    def _():
        hidden = jnp.maximum(pre_ref[...] + bias_ref[...], 0.0)
        inv = lax.rsqrt(jnp.mean(hidden * hidden, axis=-1, keepdims=True) + 0.25)
        embed = (hidden * inv).astype(jnp.bfloat16)
        embed_ref[...] = embed
        scaled[...] = embed * jnp.bfloat16(0.25)
    for part in range(2):
        cols = pl.ds(part * 512, 512)
        scores = lax.dot_general(
            scaled[...], queries_ref[cols, :], (((1,), (1,)), ((), ())), preferred_element_type=jnp.float32
        ) - logc_ref[...]
        peak = jnp.max(scores, axis=0, keepdims=True)
        total = jnp.sum(jnp.exp(scores - peak), axis=0, keepdims=True)
        stats_ref[0, 0:1, cols] = peak
        stats_ref[0, 1:2, cols] = total


def score(pre, bias, log_count, queries):
    return pl.pallas_call(
        score_kernel,
        grid=(8,),
        out_shape=(
            jax.ShapeDtypeStruct((512, 512), jnp.bfloat16),
            jax.ShapeDtypeStruct((8, 2, 1024), jnp.float32),
        ),
        in_specs=[
            pl.BlockSpec((512, 512), lambda i: (0, 0)),
            pl.BlockSpec((1, 512), lambda i: (0, 0)),
            pl.BlockSpec((512, 1), lambda i: (0, 0)),
            pl.BlockSpec((1024, 512), lambda i: (i, 0)),
        ],
        out_specs=(
            pl.BlockSpec((512, 512), lambda i: (0, 0)),
            pl.BlockSpec((1, 2, 1024), lambda i: (i, 0, 0)),
        ),
        scratch_shapes=[pltpu.VMEM((512, 512), jnp.bfloat16)],
        compiler_params=pltpu.CompilerParams(dimension_semantics=("arbitrary",), vmem_limit_bytes=32 * 1024 * 1024),
        name="score",
    )(pre, bias, log_count, queries)


def joined(stats):
    peak = jnp.max(stats[:, 0:1, :], axis=0)
    total = jnp.sum(stats[:, 1:2, :] * jnp.exp(stats[:, 0:1, :] - peak[None]), axis=0)
    return peak, total


def combine_kernel(stats_ref, out_ref, got, mine, final, send_sem, recv_sem, send_sem2, recv_sem2):
    q = lax.axis_index("qry")
    n = lax.axis_index("neg")
    row_peers = [{"qry": lax.rem(q + d, 8)} for d in range(1, 8)]
    column_peers = [{"neg": lax.rem(n + d, 16)} for d in range(1, 16)]
    greet(row_peers + column_peers)
    copies = []
    for d, peer in enumerate(row_peers):
        copies.append(remote(stats_ref.at[lax.rem(q + d + 1, 8)], got.at[q], send_sem.at[d], recv_sem.at[d], peer))
        copies[-1].start()
    got[q] = stats_ref[q]
    for copy in copies:
        copy.wait_recv()
    peak, total = joined(got[...])
    mine[...] = jnp.concatenate([peak, total], axis=0)
    final[n] = mine[...]
    for d, peer in enumerate(column_peers):
        copies.append(remote(mine, final.at[n], send_sem2.at[d], recv_sem2.at[d], peer))
        copies[-1].start()
    for copy in copies[7:]:
        copy.wait_recv()
    peak, total = joined(final[...])
    out_ref[...] = peak + jnp.log(total) - math.log(65536)
    for copy in copies:
        copy.wait_send()


def combine(stats):
    return pl.pallas_call(
        combine_kernel,
        out_shape=jax.ShapeDtypeStruct((1, 1024), jnp.float32),
        in_specs=[VMEM],
        out_specs=VMEM,
        scratch_shapes=[
            pltpu.VMEM((8, 2, 1024), jnp.float32),
            pltpu.VMEM((2, 1024), jnp.float32),
            pltpu.VMEM((16, 2, 1024), jnp.float32),
            pltpu.SemaphoreType.DMA((7,)),
            pltpu.SemaphoreType.DMA((7,)),
            pltpu.SemaphoreType.DMA((15,)),
            pltpu.SemaphoreType.DMA((15,)),
        ],
        compiler_params=pltpu.CompilerParams(collective_id=3, has_side_effects=True),
        name="combine",
    )(stats)


def per_device(
    items_table,
    fetch_rows,
    neighbour_slots,
    neighbour_count,
    self_slot,
    negative_count,
    message_weight,
    message_bias,
    self_weight,
    neighbour_weight,
    output_bias,
    queries,
):
    queries_all = lax.all_gather(queries, "qry", axis=0, tiled=True)
    last = (self_slot | jnp.left_shift(neighbour_count, 16)).reshape(1, 512)
    rows, aux = exchange_indices(fetch_rows.reshape(16, 1, 640), neighbour_slots.T, last)
    partial = partials(
        lambda: lax.axis_index("neg"), rows.reshape(16, 640), aux, items_table,
        message_weight, self_weight, neighbour_weight, message_bias.reshape(1, 512))
    pre = reduce_partials(partial)
    own_count = lax.dynamic_slice(negative_count, (lax.axis_index("qry") * 512,), (512,))
    log_count = jnp.log(own_count.astype(jnp.float32)).reshape(512, 1)
    negative_embed, stats = score(pre, output_bias.reshape(1, 512), log_count, queries_all)
    query_lse = combine(stats)
    return negative_embed, query_lse.reshape(1024)


def solution(mesh):
    in_specs = (
        P("neg", None),
        P(("neg", "qry"), None),
        P(("neg", "qry"), None),
        P(("neg", "qry")),
        P(("neg", "qry")),
        P("neg"),
        P(),
        P(),
        P(),
        P(),
        P(),
        P("qry", None),
    )
    out_specs = (P(("neg", "qry"), None), P("qry"))
    return jax.shard_map(
        per_device, mesh=mesh, in_specs=in_specs, out_specs=out_specs, check_vma=False
    )
```

```python
import functools
import math

import jax
import jax.numpy as jnp
from jax import lax
from jax.experimental import pallas as pl
from jax.experimental.pallas import tpu as pltpu
from jax.sharding import PartitionSpec as P

MESH = pl.DeviceIdType.MESH
VMEM = pl.BlockSpec(memory_space=pltpu.VMEM)


def greet(peers):
    barrier = pltpu.get_barrier_semaphore()
    for peer in peers:
        pl.semaphore_signal(barrier, inc=1, device_id=peer, device_id_type=MESH)
    pl.semaphore_wait(barrier, len(peers))


def remote(src, dst, send, recv, peer):
    return pltpu.make_async_remote_copy(
        src_ref=src, dst_ref=dst, send_sem=send, recv_sem=recv, device_id=peer, device_id_type=MESH
    )


def build_table(table_ref, wm_ref, ws_ref, wn_ref, bm_ref, t_ref, tbuf, in_sem):
    blk = 512
    blocks = 16

    def fetch(i, slot):
        return pltpu.make_async_copy(table_ref.at[pl.ds(i * blk, blk), :], tbuf.at[slot], in_sem.at[slot])

    fetch(0, 0).start()

    def build(i, _):
        slot = lax.rem(i, 2)

        @pl.when(i + 1 < blocks)
        def _():
            fetch(i + 1, 1 - slot).start()
        fetch(i, slot).wait()
        x = tbuf[slot]
        m = jnp.dot(x, wm_ref[...], preferred_element_type=jnp.float32) + bm_ref[...]
        m = jnp.maximum(m, 0.0).astype(jnp.bfloat16)
        t1 = jnp.dot(m, wn_ref[...], preferred_element_type=jnp.float32)
        t2 = jnp.dot(x, ws_ref[...], preferred_element_type=jnp.float32)
        base = pl.multiple_of(i * (blk * 8), 8)
        flat = t_ref.reshape(65536, 128)
        for j in range(4):
            flat[pl.ds(base + j, blk, stride=8), :] = t1[:, j * 128:(j + 1) * 128]
            flat[pl.ds(base + 4 + j, blk, stride=8), :] = t2[:, j * 128:(j + 1) * 128]
        return 0
    lax.fori_loop(0, blocks, build, 0)


GROUPS = ((0, 7), (7, 14), (14, 21), (21, 28), (28, 34), (34, 40))


def prepare(n, p, rows_ref, aux_ref, t_ref, g_ref, self_ref, rcnt_ref, key_ref, val_ref, gb_ref, c_ref, rc_ref):
    packed = aux_ref[n]
    for h, slots in enumerate((packed & 0xFFFF, lax.shift_right_logical(packed, 16))):
        rel = slots - 640 * p
        ok = (rel >= 0) & (rel < 640)
        key_ref[h * 24:(h + 1) * 24, :] = rel & 63
        shift = 3 * jnp.where(ok, lax.shift_right_logical(rel, 6), 0)
        val_ref[h * 24:(h + 1) * 24, :] = jnp.where(ok, jnp.left_shift(1, shift), 0)
    sub = lax.broadcasted_iota(jnp.int32, (64, 128), 0)
    lane = lax.broadcasted_iota(jnp.int32, (128, 128), 1)
    here = lane == n
    even = 0o0707070707
    for vb in range(4):
        for s in range(vb * 160, vb * 160 + 160):
            r = rows_ref[n * 640 + s]
            g_ref[s * 8:s * 8 + 8, :] = t_ref[r]
        cols = slice(vb * 128, (vb + 1) * 128)
        low = jnp.zeros((64, 128), jnp.int32)
        high = jnp.zeros((64, 128), jnp.int32)
        for first, last in GROUPS:
            acc = jnp.zeros((64, 128), jnp.int32)
            for k in range(first, last):
                kk = k if k < 20 else k + 4
                key = jnp.broadcast_to(key_ref[kk:kk + 1, cols], (64, 128))
                val = jnp.broadcast_to(val_ref[kk:kk + 1, cols], (64, 128))
                acc = acc + jnp.where(sub == key, val, 0)
            low = low + (acc & even)
            high = high + (lax.shift_right_logical(acc, 3) & even)
        ct = jnp.concatenate([low, high], axis=0).T
        self_col = jnp.sum(jnp.where(here, self_ref[cols, :], 0.0), axis=1, keepdims=True).astype(jnp.int32) - 640 * p
        rc_ref[cols, :] = jnp.sum(jnp.where(here, rcnt_ref[cols, :], 0.0), axis=1, keepdims=True)
        for f in range(5):
            c_ref[cols, f * 128:(f + 1) * 128] = (lax.shift_right_logical(ct, 6 * f) & 63).astype(jnp.float32).astype(jnp.bfloat16)
            c_ref[cols, 640 + f * 128:640 + (f + 1) * 128] = jnp.where(self_col == lane + f * 128, 1.0, 0.0).astype(jnp.bfloat16)
        for j in range(8):
            gb_ref[vb * 160:vb * 160 + 160, j * 128:(j + 1) * 128] = g_ref[pl.ds(vb * 1280 + j, 160, stride=8), :].astype(jnp.bfloat16)


def multiply(gb_ref, c_ref, rc_ref):
    part = jnp.dot(c_ref[:, :640], gb_ref[:, :512], preferred_element_type=jnp.float32) * rc_ref[...]
    part = part + jnp.dot(c_ref[:, 640:], gb_ref[:, 512:], preferred_element_type=jnp.float32)
    return part.astype(jnp.bfloat16)


ORDER = ((2, 2), (2, 1), (1, 2), (2, 3), (3, 2), (2, 0), (0, 2), (1, 1),
         (3, 3), (1, 3), (3, 1), (1, 0), (0, 1), (3, 0), (0, 3), (0, 0))
PLACE = {pair: i for i, pair in enumerate(ORDER)}
CODE = tuple(sum(pair[axis] * 4 ** i for i, pair in enumerate(ORDER)) for axis in range(2))


def tower_kernel(fetch_ref, slots_ref, count_ref, slot_ref, table_ref, wm_ref, ws_ref, wn_ref, bm_ref, queries_ref,
                 pre_ref, all_ref,
                 t_ref, tbuf, g_ref, gb0, gb1, c0, c1, rc0, rc1, key_ref, val_ref, self_ref, rcnt_ref, p_ref,
                 rows_own, rows_got, rows_sm, aux_own, aux, near, far, near2, far2,
                 in_sem, row_send, row_recv, aux_send, aux_recv, sm_sem, own_sem, q_send, q_recv,
                 send1, recv1, send2, recv2):
    me = lax.axis_index("neg")
    q = lax.axis_index("qry")
    spot = (me // 4, lax.rem(me, 4))
    peers = [{"neg": lax.rem(me + d, 16)} for d in range(1, 16)]
    above, below = lax.rem(q + 2, 8), lax.rem(q + 6, 8)
    partner = q + 1 - 2 * lax.rem(q, 2)
    across = lax.rem(q + 4, 8)

    def device(axis, step):
        moved = lax.rem(spot[axis] + step + 4, 4)
        return {"neg": moved * 4 + spot[1] if axis == 0 else spot[0] * 4 + moved}

    for j in range(16):
        rows_own[j] = fetch_ref[j:j + 1, :]
    count = count_ref[...]
    for h in range(2):
        ks = lax.broadcasted_iota(jnp.int32, (20, 512), 0) + 20 * h
        half = jnp.where(ks < count, slots_ref[20 * h:20 * h + 20, :], 0xFFFF)
        if h == 0:
            low = half
        else:
            aux_own[0:20, :] = low | jnp.left_shift(half, 16)
    aux_own[20:24, :] = jnp.broadcast_to(slot_ref[...] | jnp.left_shift(count, 16), (4, 512))

    greet(peers + [{"qry": above}, {"qry": below}, {"qry": partner}])
    row_copies = []
    aux_copies = []
    for d, peer in enumerate(peers):
        other = lax.rem(me + d + 1, 16)
        row_copies.append(remote(rows_own.at[other], rows_got.at[me], row_send.at[d], row_recv.at[d], peer))
    for d, peer in enumerate(peers):
        aux_copies.append(remote(aux_own, aux.at[me], aux_send.at[d], aux_recv.at[d], peer))
    for copy in row_copies + aux_copies:
        copy.start()
    rows_got[me] = rows_own[me]
    aux[me] = aux_own[...]

    def pass_on(i, source, place, size, peer):
        return remote(source, all_ref.at[pl.ds(place, size), :], q_send.at[i], q_recv.at[i], {"qry": peer})

    own_copy = pltpu.make_async_copy(queries_ref, all_ref.at[pl.ds(q * 1024, 1024), :], own_sem)
    spread = [pass_on(i, queries_ref, q * 1024, 1024, peer) for i, peer in enumerate((above, below, partner))]

    def held(i, place, size, peer):
        return pass_on(i, all_ref.at[pl.ds(place, size), :], place, size, peer)

    relay = [
        held(3, below * 1024, 512, above),
        held(4, above * 1024 + 512, 512, below),
        held(5, below * 1024, 1024, partner),
        held(6, above * 1024, 1024, partner),
    ]
    hand = [held(7, across * 1024, 512, partner), held(8, across * 1024 + 512, 512, partner)]
    own_copy.start()
    for copy in spread:
        copy.start()

    build_table(table_ref, wm_ref, ws_ref, wn_ref, bm_ref, t_ref, tbuf, in_sem)

    for copy in row_copies:
        copy.wait_recv()
    to_scalar = [
        pltpu.make_async_copy(rows_got.at[j, 0], rows_sm.at[pl.ds(j * 640, 640)], sm_sem.at[j]) for j in range(16)
    ]
    for copy in to_scalar:
        copy.start()
    for copy in aux_copies:
        copy.wait_recv()
    last = aux[:, 20, :]
    last = jnp.concatenate([last] * 8, axis=0)
    self_ref[...] = (last & 0xFFFF).astype(jnp.float32).T
    rcnt_ref[...] = (1.0 / lax.shift_right_logical(last, 16).astype(jnp.float32)).T
    for copy in to_scalar:
        copy.wait()

    def near_copy(half, w, j):
        pair = (2, j) if half == 0 else (j, 2)
        rows = pl.ds(256 * half + 128 * w, 128)
        return remote(p_ref.at[PLACE[pair], rows, :], near.at[half, w, j],
                      send1.at[half, w, 0, j], recv1.at[half, w, 0, j], device(half, 1 - 2 * w))

    def far_copy(half, w, stage, j):
        side = 1 + 2 * w
        pair = (side, j) if half == 0 else (j, side)
        part = w if stage == 2 else 1 - w
        rows = pl.ds(256 * half + 128 * part, 128)
        return remote(p_ref.at[PLACE[pair], rows, :], far.at[half, w, 2 - stage, j],
                      send1.at[half, w, stage, j], recv1.at[half, w, stage, j], device(half, 1 - 2 * w))

    def send_place(c):
        for half in range(2):
            d, j = ORDER[c][half], ORDER[c][1 - half]
            if d == 2:
                for w in range(2):
                    near_copy(half, w, j).start()
            elif d != 0:
                far_copy(half, (d - 1) // 2, 1, j).start()

    def step(dx, dy, gb, c, rc):
        n = lax.rem(spot[0] + dx, 4) * 4 + lax.rem(spot[1] + dy, 4)
        prepare(n, me, rows_sm, aux, t_ref, g_ref, self_ref, rcnt_ref, key_ref, val_ref, gb, c, rc)

    step(ORDER[0][0], ORDER[0][1], gb0, c0, rc0)

    def two(i, codes):
        cx, cy = codes
        step(lax.rem(cx, 4), lax.rem(cy, 4), gb1, c1, rc1)
        p_ref[2 * i] = multiply(gb0, c0, rc0)
        for place in range(8):
            @pl.when(i == place)
            def _():
                send_place(2 * place)
        cx, cy = cx // 4, cy // 4
        step(lax.rem(cx, 4), lax.rem(cy, 4), gb0, c0, rc0)
        p_ref[2 * i + 1] = multiply(gb1, c1, rc1)
        for place in range(8):
            @pl.when(i == place)
            def _():
                send_place(2 * place + 1)
        return cx // 4, cy // 4
    lax.fori_loop(0, 8, two, (jnp.int32(CODE[0] // 4), jnp.int32(CODE[1] // 4)))

    f32 = jnp.float32
    for copy in spread:
        copy.wait_recv()
    for copy in relay:
        copy.start()

    for j in (2, 1, 3, 0):
        for half in range(2):
            for w in range(2):
                near_copy(half, w, j).wait_recv()
                side = 1 + 2 * w
                pair = (side, j) if half == 0 else (j, side)
                rows = slice(256 * half + 128 * w, 256 * half + 128 * w + 128)
                value = p_ref[PLACE[pair], rows, :].astype(f32) + near[half, w, j].astype(f32)
                p_ref[PLACE[pair], rows, :] = value.astype(jnp.bfloat16)
                far_copy(half, w, 2, j).start()

    def home_at(half, j, part):
        first = 256 * half + 128 * part
        return PLACE[(0, j) if half == 0 else (j, 0)], slice(first, first + 128), slice(None)

    def second_copy(half, w, stage):
        target = (near2.at[half, w], far2.at[half, w, 1], far2.at[half, w, 0])[stage]
        return remote(p_ref.at[home_at(half, (2, 1 + 2 * w, 1 + 2 * w)[stage], (w, 1 - w, w)[stage])], target, send2.at[half, w, stage], recv2.at[half, w, stage],
                      device(1 - half, 1 - 2 * w))

    def total_at(half, j, part, c):
        first = (((half * 4 + j) * 2 + part) * 4 + c) * 16
        return slice(first, first + 16), slice(None), slice(None)

    for j in (2, 1, 3, 0):
        for half in range(2):
            for part in range(2):
                far_copy(half, part, 2, j).wait_recv()
                far_copy(half, part, 1, j).wait_recv()
        for half in range(2):
            for part in range(2):
                value = p_ref[home_at(half, j, part)].astype(f32) + far[half, part, 0, j].astype(f32)
                value = value + far[half, 1 - part, 1, j].astype(f32)
                if j == 2:
                    p_ref[home_at(half, j, part)] = value.astype(jnp.bfloat16)
                    second_copy(half, part, 0).start()
                    continue
                if j != 0 and part == 1 - (j - 1) // 2:
                    p_ref[home_at(half, j, part)] = value.astype(jnp.bfloat16)
                    second_copy(half, 1 - part, 1).start()
                    continue
                for c in range(4):
                    t_ref[total_at(half, j, part, c)] = value[:, c * 128:(c + 1) * 128].reshape(16, 8, 128)
    for half in range(2):
        for w in range(2):
            second_copy(half, w, 0).wait_recv()
            for c in range(4):
                lanes = slice(c * 128, (c + 1) * 128)
                value = t_ref[total_at(half, 1 + 2 * w, w, c)].reshape(128, 128) + near2[half, w, :, lanes].astype(f32)
                place, rows, _ = home_at(half, 1 + 2 * w, w)
                p_ref[place, rows, lanes] = value.astype(jnp.bfloat16)
            second_copy(half, w, 2).start()
    for copy in relay:
        copy.wait_recv()
    for copy in hand:
        copy.start()
    for half in range(2):
        for w in range(2):
            second_copy(half, w, 1).wait_recv()
            second_copy(half, w, 2).wait_recv()
        for w in range(2):
            rows = slice(256 * half + 128 * w, 256 * half + 128 * w + 128)
            for c in range(4):
                lanes = slice(c * 128, (c + 1) * 128)
                value = t_ref[total_at(half, 0, w, c)].reshape(128, 128) + far2[half, w, 0, :, lanes].astype(f32)
                pre_ref[rows, lanes] = value + far2[half, 1 - w, 1, :, lanes].astype(f32)
    own_copy.wait()
    for copy in hand:
        copy.wait_recv()
    for copy in row_copies + aux_copies + spread + relay + hand:
        copy.wait_send()
    for half in range(2):
        for w in range(2):
            for j in range(4):
                near_copy(half, w, j).wait_send()
                far_copy(half, w, 1, j).wait_send()
                far_copy(half, w, 2, j).wait_send()
            for stage in range(3):
                second_copy(half, w, stage).wait_send()


def tower(fetch_rows, slots, count, slot, table, wm, ws, wn, bm, queries):
    any_space = pl.BlockSpec(memory_space=pl.ANY)
    bf16, f32, i32 = jnp.bfloat16, jnp.float32, jnp.int32
    dma = pltpu.SemaphoreType.DMA
    return pl.pallas_call(
        tower_kernel,
        out_shape=(
            jax.ShapeDtypeStruct((512, 512), f32),
            jax.ShapeDtypeStruct((8192, 512), bf16),
        ),
        in_specs=[VMEM] * 4 + [any_space] + [VMEM] * 4 + [any_space],
        out_specs=(VMEM, any_space),
        scratch_shapes=[
            pltpu.VMEM((8192, 8, 128), f32),
            pltpu.VMEM((2, 512, 512), bf16),
            pltpu.VMEM((5120, 128), f32),
            pltpu.VMEM((640, 1024), bf16),
            pltpu.VMEM((640, 1024), bf16),
            pltpu.VMEM((512, 1280), bf16),
            pltpu.VMEM((512, 1280), bf16),
            pltpu.VMEM((512, 1), f32),
            pltpu.VMEM((512, 1), f32),
            pltpu.VMEM((48, 512), i32),
            pltpu.VMEM((48, 512), i32),
            pltpu.VMEM((512, 128), f32),
            pltpu.VMEM((512, 128), f32),
            pltpu.VMEM((16, 512, 512), bf16),
            pltpu.VMEM((16, 1, 640), i32),
            pltpu.VMEM((16, 1, 640), i32),
            pltpu.SMEM((10240,), i32),
            pltpu.VMEM((24, 512), i32),
            pltpu.VMEM((16, 24, 512), i32),
            pltpu.VMEM((2, 2, 4, 128, 512), bf16),
            pltpu.VMEM((2, 2, 2, 4, 128, 512), bf16),
            pltpu.VMEM((2, 2, 128, 512), bf16),
            pltpu.VMEM((2, 2, 2, 128, 512), bf16),
            dma((2,)),
            dma((15,)), dma((15,)), dma((15,)), dma((15,)),
            dma((16,)), dma, dma((9,)), dma((9,)),
            dma((2, 2, 3, 4)), dma((2, 2, 3, 4)), dma((2, 2, 3)), dma((2, 2, 3)),
        ],
        compiler_params=pltpu.CompilerParams(
            collective_id=1, has_side_effects=True, vmem_limit_bytes=67043328),
        name="tower",
    )(fetch_rows, slots, count, slot, table, wm, ws, wn, bm, queries)


def joined(stats):
    peak = jnp.max(stats[:, 0:1, :], axis=0)
    total = jnp.sum(stats[:, 1:2, :] * jnp.exp(stats[:, 0:1, :] - peak[None]), axis=0)
    return peak, total


def score_kernel(pre_ref, bias_ref, logc_ref, queries_ref, embed_ref, lse_ref,
                 scaled, qbuf, stats, got, mine, final, in_sem, send_sem, recv_sem, send_sem2, recv_sem2):
    q = lax.axis_index("qry")
    n = lax.axis_index("neg")
    row_peers = [{"qry": lax.rem(q + d, 8)} for d in range(1, 8)]
    column_peers = [{"neg": lax.rem(n + d, 16)} for d in range(1, 16)]

    def fetch(d):
        block = lax.rem(q + d, 8)
        return pltpu.make_async_copy(queries_ref.at[pl.ds(block * 1024, 1024), :], qbuf.at[d - 1], in_sem.at[d - 1])

    for d in range(1, 9):
        fetch(d).start()
    hidden = jnp.maximum(pre_ref[...] + bias_ref[...], 0.0)
    inv = lax.rsqrt(jnp.mean(hidden * hidden, axis=-1, keepdims=True) + 0.25)
    embed = (hidden * inv).astype(jnp.bfloat16)
    embed_ref[...] = embed
    scaled[...] = embed * jnp.bfloat16(0.25)
    greet(row_peers + column_peers)

    def block_copy(i, d):
        return remote(stats.at[i], got.at[q], send_sem.at[d - 1], recv_sem.at[d - 1], {"qry": lax.rem(q + d, 8)})

    def block(i, _):
        pltpu.make_async_copy(queries_ref.at[pl.ds(lax.rem(q + i + 1, 8) * 1024, 1024), :], qbuf.at[i], in_sem.at[i]).wait()
        for part in range(2):
            cols = pl.ds(part * 512, 512)
            scores = lax.dot_general(
                scaled[...], qbuf[i, cols, :], (((1,), (1,)), ((), ())), preferred_element_type=jnp.float32
            ) - logc_ref[...]
            peak = jnp.max(scores, axis=0, keepdims=True)
            total = jnp.sum(jnp.exp(scores - peak), axis=0, keepdims=True)
            stats[i, 0:1, cols] = peak
            stats[i, 1:2, cols] = total
        for d in range(1, 8):
            @pl.when(i == d - 1)
            def _():
                block_copy(d - 1, d).start()
        return 0
    lax.fori_loop(0, 8, block, 0)
    got[q] = stats[7]
    copies = [block_copy(d - 1, d) for d in range(1, 8)]
    for copy in copies:
        copy.wait_recv()
    peak, total = joined(got[...])
    mine[...] = jnp.concatenate([peak, total], axis=0)
    final[n] = mine[...]
    for d, peer in enumerate(column_peers):
        copies.append(remote(mine, final.at[n], send_sem2.at[d], recv_sem2.at[d], peer))
        copies[-1].start()
    for copy in copies[7:]:
        copy.wait_recv()
    peak, total = joined(final[...])
    lse_ref[...] = peak + jnp.log(total) - math.log(65536)
    for copy in copies:
        copy.wait_send()


def score(pre, bias, log_count, queries):
    f32 = jnp.float32
    dma = pltpu.SemaphoreType.DMA
    return pl.pallas_call(
        score_kernel,
        out_shape=(
            jax.ShapeDtypeStruct((512, 512), jnp.bfloat16),
            jax.ShapeDtypeStruct((1, 1024), f32),
        ),
        in_specs=[VMEM, VMEM, VMEM, pl.BlockSpec(memory_space=pl.ANY)],
        out_specs=(VMEM, VMEM),
        scratch_shapes=[
            pltpu.VMEM((512, 512), jnp.bfloat16),
            pltpu.VMEM((8, 1024, 512), jnp.bfloat16),
            pltpu.VMEM((8, 2, 1024), f32),
            pltpu.VMEM((8, 2, 1024), f32),
            pltpu.VMEM((2, 1024), f32),
            pltpu.VMEM((16, 2, 1024), f32),
            dma((8,)), dma((7,)), dma((7,)), dma((15,)), dma((15,)),
        ],
        compiler_params=pltpu.CompilerParams(
            collective_id=2, has_side_effects=True, vmem_limit_bytes=48 * 1024 * 1024),
        name="score",
    )(pre, bias, log_count, queries)


def per_device(
    items_table,
    fetch_rows,
    neighbour_slots,
    neighbour_count,
    self_slot,
    negative_count,
    message_weight,
    message_bias,
    self_weight,
    neighbour_weight,
    output_bias,
    queries,
):
    own_count = lax.dynamic_slice(negative_count, (lax.axis_index("qry") * 512,), (512,))
    log_count = jnp.log(own_count.astype(jnp.float32)).reshape(512, 1)
    pre, queries_all = tower(
        fetch_rows, neighbour_slots.T, neighbour_count.reshape(1, 512), self_slot.reshape(1, 512), items_table,
        message_weight, self_weight, neighbour_weight, message_bias.reshape(1, 512), queries)
    negative_embed, query_lse = score(pre, output_bias.reshape(1, 512), log_count, queries_all)
    return negative_embed, query_lse.reshape(1024)


def solution(mesh):
    in_specs = (
        P("neg", None),
        P(("neg", "qry"), None),
        P(("neg", "qry"), None),
        P(("neg", "qry")),
        P(("neg", "qry")),
        P("neg"),
        P(),
        P(),
        P(),
        P(),
        P(),
        P("qry", None),
    )
    out_specs = (P(("neg", "qry"), None), P("qry"))
    return jax.shard_map(
        per_device, mesh=mesh, in_specs=in_specs, out_specs=out_specs, check_vma=False
    )
```

```python
import functools
import math

import jax
import jax.numpy as jnp
from jax import lax
from jax.experimental import pallas as pl
from jax.experimental.pallas import tpu as pltpu
from jax.sharding import PartitionSpec as P

MESH = pl.DeviceIdType.MESH
VMEM = pl.BlockSpec(memory_space=pltpu.VMEM)


def greet(peers):
    barrier = pltpu.get_barrier_semaphore()
    for peer in peers:
        pl.semaphore_signal(barrier, inc=1, device_id=peer, device_id_type=MESH)
    pl.semaphore_wait(barrier, len(peers))


def remote(src, dst, send, recv, peer):
    return pltpu.make_async_remote_copy(
        src_ref=src, dst_ref=dst, send_sem=send, recv_sem=recv, device_id=peer, device_id_type=MESH
    )


def build_table(table_ref, wm_ref, ws_ref, wn_ref, bm_ref, t_ref, tbuf, in_sem):
    blk = 512
    blocks = 16

    def fetch(i, slot):
        return pltpu.make_async_copy(table_ref.at[pl.ds(i * blk, blk), :], tbuf.at[slot], in_sem.at[slot])

    fetch(0, 0).start()

    def build(i, _):
        slot = lax.rem(i, 2)

        @pl.when(i + 1 < blocks)
        def _():
            fetch(i + 1, 1 - slot).start()
        fetch(i, slot).wait()
        x = tbuf[slot]
        m = jnp.dot(x, wm_ref[...], preferred_element_type=jnp.float32) + bm_ref[...]
        m = jnp.maximum(m, 0.0).astype(jnp.bfloat16)
        t1 = jnp.dot(m, wn_ref[...], preferred_element_type=jnp.float32)
        t2 = jnp.dot(x, ws_ref[...], preferred_element_type=jnp.float32)
        base = pl.multiple_of(i * (blk * 8), 8)
        flat = t_ref.reshape(65536, 128)
        for j in range(4):
            flat[pl.ds(base + j, blk, stride=8), :] = t1[:, j * 128:(j + 1) * 128]
            flat[pl.ds(base + 4 + j, blk, stride=8), :] = t2[:, j * 128:(j + 1) * 128]
        return 0
    lax.fori_loop(0, blocks, build, 0)


GROUPS = ((0, 7), (7, 14), (14, 21), (21, 28), (28, 34), (34, 40))


def prepare(n, p, rows_ref, aux_ref, t_ref, g_ref, self_ref, rcnt_ref, key_ref, val_ref, gb_ref, c_ref, rc_ref):
    packed = aux_ref[n]
    for h, slots in enumerate((packed & 0xFFFF, lax.shift_right_logical(packed, 16))):
        rel = slots - 640 * p
        ok = (rel >= 0) & (rel < 640)
        key_ref[h * 24:(h + 1) * 24, :] = rel & 63
        shift = 3 * jnp.where(ok, lax.shift_right_logical(rel, 6), 0)
        val_ref[h * 24:(h + 1) * 24, :] = jnp.where(ok, jnp.left_shift(1, shift), 0)
    sub = lax.broadcasted_iota(jnp.int32, (64, 128), 0)
    lane = lax.broadcasted_iota(jnp.int32, (128, 128), 1)
    here = lane == n
    even = 0o0707070707
    for vb in range(4):
        for s in range(vb * 160, vb * 160 + 160):
            r = rows_ref[n * 640 + s]
            g_ref[s * 8:s * 8 + 8, :] = t_ref[r]
        cols = slice(vb * 128, (vb + 1) * 128)
        low = jnp.zeros((64, 128), jnp.int32)
        high = jnp.zeros((64, 128), jnp.int32)
        for first, last in GROUPS:
            acc = jnp.zeros((64, 128), jnp.int32)
            for k in range(first, last):
                kk = k if k < 20 else k + 4
                key = jnp.broadcast_to(key_ref[kk:kk + 1, cols], (64, 128))
                val = jnp.broadcast_to(val_ref[kk:kk + 1, cols], (64, 128))
                acc = acc + jnp.where(sub == key, val, 0)
            low = low + (acc & even)
            high = high + (lax.shift_right_logical(acc, 3) & even)
        ct = jnp.concatenate([low, high], axis=0).T
        self_col = jnp.sum(jnp.where(here, self_ref[cols, :], 0.0), axis=1, keepdims=True).astype(jnp.int32) - 640 * p
        rc_ref[cols, :] = jnp.sum(jnp.where(here, rcnt_ref[cols, :], 0.0), axis=1, keepdims=True)
        for f in range(5):
            c_ref[cols, f * 128:(f + 1) * 128] = (lax.shift_right_logical(ct, 6 * f) & 63).astype(jnp.float32).astype(jnp.bfloat16)
            c_ref[cols, 640 + f * 128:640 + (f + 1) * 128] = jnp.where(self_col == lane + f * 128, 1.0, 0.0).astype(jnp.bfloat16)
        for j in range(8):
            gb_ref[vb * 160:vb * 160 + 160, j * 128:(j + 1) * 128] = g_ref[pl.ds(vb * 1280 + j, 160, stride=8), :].astype(jnp.bfloat16)


def multiply(gb_ref, c_ref, rc_ref):
    part = jnp.dot(c_ref[:, :640], gb_ref[:, :512], preferred_element_type=jnp.float32) * rc_ref[...]
    part = part + jnp.dot(c_ref[:, 640:], gb_ref[:, 512:], preferred_element_type=jnp.float32)
    return part.astype(jnp.bfloat16)


ORDER = ((2, 2), (1, 2), (3, 2), (2, 1), (2, 3), (1, 1), (3, 3), (2, 0),
         (0, 2), (1, 3), (3, 1), (1, 0), (0, 1), (3, 0), (0, 3), (0, 0))
PLACE = {pair: i for i, pair in enumerate(ORDER)}
CODE = tuple(sum(pair[axis] * 4 ** i for i, pair in enumerate(ORDER)) for axis in range(2))


CARRY_AT = {
    (0, 0, 2): 3, (0, 1, 2): 3, (1, 0, 2): 4, (1, 1, 2): 4, (0, 0, 1): 7, (0, 1, 1): 10, (0, 0, 3): 9, (0, 1, 3): 8,
    (1, 0, 1): 6, (1, 1, 1): 9, (1, 0, 3): 10, (1, 1, 3): 7, (0, 0, 0): 11, (0, 1, 0): 13, (1, 0, 0): 12, (1, 1, 0): 14,
}
HOME_AT = {(0, 2): 8, (1, 2): 9, (1, 1): 13, (0, 1): 14, (0, 3): 14, (1, 3): 14}
RELAY_AT, HAND_AT = 5, 12

def tower_kernel(fetch_ref, slots_ref, count_ref, slot_ref, table_ref, wm_ref, ws_ref, wn_ref, bm_ref, bias_ref,
                 sampled_ref, queries_ref,
                 embed_ref, lse_ref, all_ref,
                 t_ref, tbuf, g_ref, gb0, gb1, c0, c1, rc0, rc1, key_ref, val_ref, self_ref, rcnt_ref, p_ref,
                 rows_own, rows_got, rows_sm, aux_own, aux, mail, near2, far2, logc_ref, stats, got, mine, final,
                 in_sem, row_send, row_recv, aux_send, aux_recv, sm_sem, own_sem, q_send, q_recv,
                 send1, recv1, send2, recv2, load_sem, send3, recv3, send4, recv4):
    me = lax.axis_index("neg")
    q = lax.axis_index("qry")
    spot = (me // 4, lax.rem(me, 4))
    peers = [{"neg": lax.rem(me + d, 16)} for d in range(1, 16)]
    above, below = lax.rem(q + 2, 8), lax.rem(q + 6, 8)
    partner = q + 1 - 2 * lax.rem(q, 2)
    across = lax.rem(q + 4, 8)

    def device(axis, step):
        moved = lax.rem(spot[axis] + step + 4, 4)
        return {"neg": moved * 4 + spot[1] if axis == 0 else spot[0] * 4 + moved}

    for j in range(16):
        rows_own[j] = fetch_ref[j:j + 1, :]
    count = count_ref[...]
    for h in range(2):
        ks = lax.broadcasted_iota(jnp.int32, (20, 512), 0) + 20 * h
        half = jnp.where(ks < count, slots_ref[20 * h:20 * h + 20, :], 0xFFFF)
        if h == 0:
            low = half
        else:
            aux_own[0:20, :] = low | jnp.left_shift(half, 16)
    aux_own[20:24, :] = jnp.broadcast_to(slot_ref[...] | jnp.left_shift(count, 16), (4, 512))

    sampled = sampled_ref[:, pl.ds(pl.multiple_of(q * 512, 128), 512)].astype(jnp.float32)
    logc_ref[...] = jnp.broadcast_to(jnp.log(sampled), (128, 512)).T

    row_peers = [{"qry": lax.rem(q + d, 8)} for d in range(1, 8)]
    greet(peers + row_peers)
    row_copies = []
    aux_copies = []
    for d, peer in enumerate(peers):
        other = lax.rem(me + d + 1, 16)
        row_copies.append(remote(rows_own.at[other], rows_got.at[me], row_send.at[d], row_recv.at[d], peer))
    for d, peer in enumerate(peers):
        aux_copies.append(remote(aux_own, aux.at[me], aux_send.at[d], aux_recv.at[d], peer))
    for copy in row_copies + aux_copies:
        copy.start()
    rows_got[me] = rows_own[me]
    aux[me] = aux_own[...]

    def pass_on(i, source, place, size, peer):
        return remote(source, all_ref.at[pl.ds(place, size)], q_send.at[i], q_recv.at[i], {"qry": peer})

    own_copy = pltpu.make_async_copy(queries_ref, all_ref.at[pl.ds(q * 2, 2)], own_sem)
    spread = [pass_on(i, queries_ref, q * 2, 2, peer) for i, peer in enumerate((above, below, partner))]

    def held(i, place, size, peer):
        return pass_on(i, all_ref.at[pl.ds(place, size)], place, size, peer)

    relay = [
        held(3, below * 2, 1, above),
        held(4, above * 2 + 1, 1, below),
        held(5, below * 2, 2, partner),
        held(6, above * 2, 2, partner),
    ]
    hand = [held(7, across * 2, 1, partner), held(8, across * 2 + 1, 1, partner)]
    own_copy.start()
    for copy in spread:
        copy.start()

    build_table(table_ref, wm_ref, ws_ref, wn_ref, bm_ref, t_ref, tbuf, in_sem)

    for copy in row_copies:
        copy.wait_recv()
    to_scalar = [
        pltpu.make_async_copy(rows_got.at[j, 0], rows_sm.at[pl.ds(j * 640, 640)], sm_sem.at[j]) for j in range(16)
    ]
    for copy in to_scalar:
        copy.start()
    for copy in aux_copies:
        copy.wait_recv()
    last = aux[:, 20, :]
    last = jnp.concatenate([last] * 8, axis=0)
    self_ref[...] = (last & 0xFFFF).astype(jnp.float32).T
    rcnt_ref[...] = (1.0 / lax.shift_right_logical(last, 16).astype(jnp.float32)).T
    for copy in to_scalar:
        copy.wait()

    def near_copy(half, w, j):
        pair = (2, j) if half == 0 else (j, 2)
        rows = pl.ds(256 * half + 128 * w, 128)
        return remote(p_ref.at[PLACE[pair], rows, :], mail.at[half * 2 + w, j],
                      send1.at[half, w, 0, j], recv1.at[half, w, 0, j], device(half, 1 - 2 * w))

    def far_copy(half, w, stage, j):
        side = 1 + 2 * w
        pair = (side, j) if half == 0 else (j, side)
        part = w if stage == 2 else 1 - w
        rows = pl.ds(256 * half + 128 * part, 128)
        return remote(p_ref.at[PLACE[pair], rows, :], mail.at[4 + (half * 2 + w) * 2 + 2 - stage, j],
                      send1.at[half, w, stage, j], recv1.at[half, w, stage, j], device(half, 1 - 2 * w))

    def send_place(c):
        for half in range(2):
            d, j = ORDER[c][half], ORDER[c][1 - half]
            if d == 2:
                for w in range(2):
                    near_copy(half, w, j).start()
            elif d != 0:
                far_copy(half, (d - 1) // 2, 1, j).start()

    def step(dx, dy, gb, c, rc):
        n = lax.rem(spot[0] + dx, 4) * 4 + lax.rem(spot[1] + dy, 4)
        prepare(n, me, rows_sm, aux, t_ref, g_ref, self_ref, rcnt_ref, key_ref, val_ref, gb, c, rc)

    f32 = jnp.float32

    def carry(half, w, j):
        near_copy(half, w, j).wait_recv()
        side = 1 + 2 * w
        pair = (side, j) if half == 0 else (j, side)
        rows = slice(256 * half + 128 * w, 256 * half + 128 * w + 128)
        value = p_ref[PLACE[pair], rows, :].astype(f32) + mail[half * 2 + w, j].astype(f32)
        p_ref[PLACE[pair], rows, :] = value.astype(jnp.bfloat16)
        far_copy(half, w, 2, j).start()

    def home_at(half, j, part):
        first = 256 * half + 128 * part
        return PLACE[(0, j) if half == 0 else (j, 0)], slice(first, first + 128), slice(None)

    def second_copy(half, w, stage):
        target = (near2.at[half, w], far2.at[half, w, 1], far2.at[half, w, 0])[stage]
        place, rows, _ = home_at(half, (2, 1 + 2 * w, 1 + 2 * w)[stage], (w, 1 - w, w)[stage])
        return remote(p_ref.at[place, rows, :], target, send2.at[half, w, stage], recv2.at[half, w, stage],
                      device(1 - half, 1 - 2 * w))

    def arrive(half, j, part):
        far_copy(half, part, 2, j).wait_recv()
        far_copy(half, 1 - part, 1, j).wait_recv()

    def total(half, j, part):
        value = p_ref[home_at(half, j, part)].astype(f32) + mail[4 + (half * 2 + part) * 2, j].astype(f32)
        return value + mail[4 + (half * 2 + 1 - part) * 2 + 1, j].astype(f32)

    def home(half, j):
        for part in range(2):
            if j == 2 or part == 1 - (j - 1) // 2:
                arrive(half, j, part)
                p_ref[home_at(half, j, part)] = total(half, j, part).astype(jnp.bfloat16)
                if j == 2:
                    second_copy(half, part, 0).start()
                else:
                    second_copy(half, 1 - part, 1).start()

    def after(c):
        send_place(c)
        for (half, w, j), at in CARRY_AT.items():
            if at == c:
                carry(half, w, j)
        for (half, j), at in HOME_AT.items():
            if at == c:
                home(half, j)
        if c == RELAY_AT:
            for copy in spread:
                copy.wait_recv()
            for copy in relay:
                copy.start()
        if c == HAND_AT:
            for copy in relay:
                copy.wait_recv()
            for copy in hand:
                copy.start()

    step(ORDER[0][0], ORDER[0][1], gb0, c0, rc0)

    def two(i, codes):
        cx, cy = codes
        step(lax.rem(cx, 4), lax.rem(cy, 4), gb1, c1, rc1)
        p_ref[2 * i] = multiply(gb0, c0, rc0)
        for place in range(8):
            @pl.when(i == place)
            def _():
                after(2 * place)
        cx, cy = cx // 4, cy // 4
        step(lax.rem(cx, 4), lax.rem(cy, 4), gb0, c0, rc0)
        p_ref[2 * i + 1] = multiply(gb1, c1, rc1)
        for place in range(8):
            @pl.when(i == place)
            def _():
                after(2 * place + 1)
        return cx // 4, cy // 4
    lax.fori_loop(0, 8, two, (jnp.int32(CODE[0] // 4), jnp.int32(CODE[1] // 4)))

    own_copy.wait()
    for copy in hand:
        copy.wait_recv()

    def load(i, slot):
        block = lax.rem(q + i + 1, 8)
        return pltpu.make_async_copy(all_ref.at[pl.ds(block * 2, 2)], mail.at[pl.ds(slot * 2, 2)], load_sem.at[slot])

    load(0, 0).start()
    load(1, 1).start()

    for half in range(2):
        for w in range(2):
            second_copy(half, w, 0).wait_recv()
            arrive(half, 1 + 2 * w, w)
            value = total(half, 1 + 2 * w, w) + near2[half, w].astype(f32)
            p_ref[home_at(half, 1 + 2 * w, w)] = value.astype(jnp.bfloat16)
            second_copy(half, w, 2).start()
    for half in range(2):
        for w in range(2):
            second_copy(half, w, 1).wait_recv()
            second_copy(half, w, 2).wait_recv()
        for w in range(2):
            rows = slice(256 * half + 128 * w, 256 * half + 128 * w + 128)
            arrive(half, 0, w)
            value = total(half, 0, w) + far2[half, w, 0].astype(f32) + far2[half, 1 - w, 1].astype(f32)
            hidden = jnp.maximum(value + bias_ref[...], 0.0)
            inv = lax.rsqrt(jnp.mean(hidden * hidden, axis=-1, keepdims=True) + 0.25)
            embed = (hidden * inv).astype(jnp.bfloat16)
            embed_ref[rows, :] = embed
            c0[rows, 0:512] = embed * jnp.bfloat16(0.25)
    for i in range(2, 6):
        load(i, i).start()

    def block_copy(d):
        return remote(stats.at[d - 1], got.at[q], send3.at[d - 1], recv3.at[d - 1], row_peers[d - 1])

    def block(i, _):
        slot = lax.rem(i, 6)
        load(i, slot).wait()
        for part in range(2):
            cols = pl.ds(part * 512, 512)
            scores = lax.dot_general(
                c0[:, 0:512], mail[2 * slot + part].reshape(512, 512), (((1,), (1,)), ((), ())),
                preferred_element_type=f32)
            scores = scores - jnp.concatenate([logc_ref[...]] * 4, axis=1)
            peak = jnp.max(scores, axis=0, keepdims=True)
            total = jnp.sum(jnp.exp(scores - peak), axis=0, keepdims=True)
            stats[i, 0:1, cols] = peak
            stats[i, 1:2, cols] = total
        for d in range(1, 8):
            @pl.when(i == d - 1)
            def _():
                block_copy(d).start()

        @pl.when(i < 2)
        def _():
            load(i + 6, slot).start()
        return 0
    lax.fori_loop(0, 8, block, 0)
    got[q] = stats[7]
    last_copies = [block_copy(d) for d in range(1, 8)]
    for copy in last_copies:
        copy.wait_recv()
    peak, total = joined(got[...])
    mine[...] = jnp.concatenate([peak, total], axis=0)
    final[me] = mine[...]
    for d, peer in enumerate(peers):
        last_copies.append(remote(mine, final.at[me], send4.at[d], recv4.at[d], peer))
        last_copies[-1].start()
    for copy in last_copies[7:]:
        copy.wait_recv()
    peak, total = joined(final[...])
    lse_ref[...] = peak + jnp.log(total) - math.log(65536)

    for copy in row_copies + aux_copies + spread + relay + hand + last_copies:
        copy.wait_send()
    for half in range(2):
        for w in range(2):
            for j in range(4):
                near_copy(half, w, j).wait_send()
                far_copy(half, w, 1, j).wait_send()
                far_copy(half, w, 2, j).wait_send()
            for stage in range(3):
                second_copy(half, w, stage).wait_send()


def joined(stats):
    peak = jnp.max(stats[:, 0:1, :], axis=0)
    total = jnp.sum(stats[:, 1:2, :] * jnp.exp(stats[:, 0:1, :] - peak[None]), axis=0)
    return peak, total


def tower(fetch_rows, slots, count, slot, table, wm, ws, wn, bm, bias, sampled, queries):
    any_space = pl.BlockSpec(memory_space=pl.ANY)
    bf16, f32, i32 = jnp.bfloat16, jnp.float32, jnp.int32
    dma = pltpu.SemaphoreType.DMA
    return pl.pallas_call(
        tower_kernel,
        out_shape=(
            jax.ShapeDtypeStruct((512, 512), bf16),
            jax.ShapeDtypeStruct((1, 1024), f32),
            jax.ShapeDtypeStruct((16, 4, 128, 512), bf16),
        ),
        in_specs=[VMEM] * 4 + [any_space] + [VMEM] * 6 + [any_space],
        out_specs=(VMEM, VMEM, any_space),
        scratch_shapes=[
            pltpu.VMEM((8192, 8, 128), f32),
            pltpu.VMEM((2, 512, 512), bf16),
            pltpu.VMEM((5120, 128), f32),
            pltpu.VMEM((640, 1024), bf16),
            pltpu.VMEM((640, 1024), bf16),
            pltpu.VMEM((512, 1280), bf16),
            pltpu.VMEM((512, 1280), bf16),
            pltpu.VMEM((512, 1), f32),
            pltpu.VMEM((512, 1), f32),
            pltpu.VMEM((48, 512), i32),
            pltpu.VMEM((48, 512), i32),
            pltpu.VMEM((512, 128), f32),
            pltpu.VMEM((512, 128), f32),
            pltpu.VMEM((16, 512, 512), bf16),
            pltpu.VMEM((16, 1, 640), i32),
            pltpu.VMEM((16, 1, 640), i32),
            pltpu.SMEM((10240,), i32),
            pltpu.VMEM((24, 512), i32),
            pltpu.VMEM((16, 24, 512), i32),
            pltpu.VMEM((12, 4, 128, 512), bf16),
            pltpu.VMEM((2, 2, 128, 512), bf16),
            pltpu.VMEM((2, 2, 2, 128, 512), bf16),
            pltpu.VMEM((512, 128), f32),
            pltpu.VMEM((8, 2, 1024), f32),
            pltpu.VMEM((8, 2, 1024), f32),
            pltpu.VMEM((2, 1024), f32),
            pltpu.VMEM((16, 2, 1024), f32),
            dma((2,)),
            dma((15,)), dma((15,)), dma((15,)), dma((15,)),
            dma((16,)), dma, dma((9,)), dma((9,)),
            dma((2, 2, 3, 4)), dma((2, 2, 3, 4)), dma((2, 2, 3)), dma((2, 2, 3)),
            dma((6,)), dma((7,)), dma((7,)), dma((15,)), dma((15,)),
        ],
        compiler_params=pltpu.CompilerParams(
            collective_id=1, has_side_effects=True, vmem_limit_bytes=67043328),
        name="tower",
    )(fetch_rows, slots, count, slot, table, wm, ws, wn, bm, bias, sampled, queries)


def per_device(
    items_table,
    fetch_rows,
    neighbour_slots,
    neighbour_count,
    self_slot,
    negative_count,
    message_weight,
    message_bias,
    self_weight,
    neighbour_weight,
    output_bias,
    queries,
):
    negative_embed, query_lse, _ = tower(
        fetch_rows, neighbour_slots.T, neighbour_count.reshape(1, 512), self_slot.reshape(1, 512), items_table,
        message_weight, self_weight, neighbour_weight, message_bias.reshape(1, 512), output_bias.reshape(1, 512),
        negative_count.reshape(1, 4096), queries.reshape(2, 4, 128, 512))
    return negative_embed, query_lse.reshape(1024)


def solution(mesh):
    in_specs = (
        P("neg", None),
        P(("neg", "qry"), None),
        P(("neg", "qry"), None),
        P(("neg", "qry")),
        P(("neg", "qry")),
        P("neg"),
        P(),
        P(),
        P(),
        P(),
        P(),
        P("qry", None),
    )
    out_specs = (P(("neg", "qry"), None), P("qry"))
    return jax.shard_map(
        per_device, mesh=mesh, in_specs=in_specs, out_specs=out_specs, check_vma=False
    )
```

```python
import functools
import math

import jax
import jax.numpy as jnp
from jax import lax
from jax.experimental import pallas as pl
from jax.experimental.pallas import tpu as pltpu
from jax.sharding import PartitionSpec as P

MESH = pl.DeviceIdType.MESH
VMEM = pl.BlockSpec(memory_space=pltpu.VMEM)


def greet(peers):
    barrier = pltpu.get_barrier_semaphore()
    for peer in peers:
        pl.semaphore_signal(barrier, inc=1, device_id=peer, device_id_type=MESH)
    pl.semaphore_wait(barrier, len(peers))


def remote(src, dst, send, recv, peer):
    return pltpu.make_async_remote_copy(
        src_ref=src, dst_ref=dst, send_sem=send, recv_sem=recv, device_id=peer, device_id_type=MESH
    )


def build_table(table_ref, wm_ref, ws_ref, wn_ref, bm_ref, t_ref, tbuf, in_sem):
    blk = 512
    blocks = 16

    def fetch(i, slot):
        return pltpu.make_async_copy(table_ref.at[pl.ds(i * blk, blk), :], tbuf.at[slot], in_sem.at[slot])

    fetch(0, 0).start()

    def build(i, _):
        slot = lax.rem(i, 2)

        @pl.when(i + 1 < blocks)
        def _():
            fetch(i + 1, 1 - slot).start()
        fetch(i, slot).wait()
        x = tbuf[slot]
        m = jnp.dot(x, wm_ref[...], preferred_element_type=jnp.float32) + bm_ref[...]
        m = jnp.maximum(m, 0.0).astype(jnp.bfloat16)
        t1 = jnp.dot(m, wn_ref[...], preferred_element_type=jnp.float32)
        t2 = jnp.dot(x, ws_ref[...], preferred_element_type=jnp.float32)
        base = pl.multiple_of(i * (blk * 8), 8)
        flat = t_ref.reshape(65536, 128)
        for j in range(4):
            flat[pl.ds(base + j, blk, stride=8), :] = t1[:, j * 128:(j + 1) * 128]
            flat[pl.ds(base + 4 + j, blk, stride=8), :] = t2[:, j * 128:(j + 1) * 128]
        return 0
    lax.fori_loop(0, blocks, build, 0)


GROUPS = ((0, 7), (7, 14), (14, 21), (21, 28), (28, 34), (34, 40))


def prepare(n, p, rows_ref, aux_ref, t_ref, g_ref, self_ref, rcnt_ref, key_ref, val_ref, gb_ref, c_ref, rc_ref, iota_ref):
    packed = aux_ref[n]
    for h, slots in enumerate((packed & 0xFFFF, lax.shift_right_logical(packed, 16))):
        rel = slots - 640 * p
        ok = (rel >= 0) & (rel < 640)
        key_ref[h * 24:(h + 1) * 24, :] = rel & 63
        shift = 3 * jnp.where(ok, lax.shift_right_logical(rel, 6), 0)
        val_ref[h * 24:(h + 1) * 24, :] = jnp.where(ok, jnp.left_shift(1, shift), 0)
    sub = lax.broadcasted_iota(jnp.int32, (64, 128), 0)
    lane = lax.broadcasted_iota(jnp.int32, (128, 128), 1)
    here = lane == n
    even = 0o0707070707
    for vb in range(4):
        for s in range(vb * 160, vb * 160 + 160):
            r = rows_ref[n * 640 + s]
            g_ref[s * 9:s * 9 + 8, :] = t_ref[r]
        cols = slice(vb * 128, (vb + 1) * 128)
        low = jnp.zeros((64, 128), jnp.int32)
        high = jnp.zeros((64, 128), jnp.int32)
        for first, last in GROUPS:
            acc = jnp.zeros((64, 128), jnp.int32)
            for k in range(first, last):
                kk = k if k < 20 else k + 4
                key = jnp.broadcast_to(key_ref[kk:kk + 1, cols], (64, 128))
                val = jnp.broadcast_to(val_ref[kk:kk + 1, cols], (64, 128))
                acc = acc + jnp.where(iota_ref[...] == key, val, 0)
            low = low + (acc & even)
            high = high + (lax.shift_right_logical(acc, 3) & even)
        ct = jnp.concatenate([low, high], axis=0).T
        self_col = jnp.sum(jnp.where(here, self_ref[cols, :], 0.0), axis=1, keepdims=True).astype(jnp.int32) - 640 * p
        rc_ref[cols, :] = jnp.sum(jnp.where(here, rcnt_ref[cols, :], 0.0), axis=1, keepdims=True)
        for f in range(5):
            c_ref[cols, f * 128:(f + 1) * 128] = (lax.shift_right_logical(ct, 6 * f) & 63).astype(jnp.float32).astype(jnp.bfloat16)
            c_ref[cols, 640 + f * 128:640 + (f + 1) * 128] = jnp.where(self_col == lane + f * 128, 1.0, 0.0).astype(jnp.bfloat16)
        for j in range(8):
            gb_ref[vb * 160:vb * 160 + 160, j * 128:(j + 1) * 128] = g_ref[pl.ds(vb * 1440 + j, 160, stride=9), :].astype(jnp.bfloat16)


def multiply(gb_ref, c_ref, rc_ref):
    part = jnp.dot(c_ref[:, :640], gb_ref[:, :512], preferred_element_type=jnp.float32) * rc_ref[...]
    part = part + jnp.dot(c_ref[:, 640:], gb_ref[:, 512:], preferred_element_type=jnp.float32)
    return part.astype(jnp.bfloat16)


ORDER = ((2, 2), (1, 2), (3, 2), (2, 1), (2, 3), (1, 1), (3, 3), (2, 0),
         (0, 2), (1, 3), (3, 1), (1, 0), (0, 1), (3, 0), (0, 3), (0, 0))
PLACE = {pair: i for i, pair in enumerate(ORDER)}
CODE = tuple(sum(pair[axis] * 4 ** i for i, pair in enumerate(ORDER)) for axis in range(2))


CARRY_AT = {
    (0, 0, 2): 3, (0, 1, 2): 3, (1, 0, 2): 4, (1, 1, 2): 4, (0, 0, 1): 7, (0, 1, 1): 10, (0, 0, 3): 9, (0, 1, 3): 8,
    (1, 0, 1): 6, (1, 1, 1): 9, (1, 0, 3): 10, (1, 1, 3): 7, (0, 0, 0): 11, (0, 1, 0): 13, (1, 0, 0): 12, (1, 1, 0): 14,
}
HOME_AT = {(0, 2): 8, (1, 2): 9, (1, 1): 13, (0, 1): 14, (0, 3): 14, (1, 3): 14}
RELAY_AT, HAND_AT = 5, 12

def tower_kernel(fetch_ref, slots_ref, count_ref, slot_ref, table_ref, wm_in, ws_in, wn_in, bm_ref, bias_ref,
                 sampled_ref, queries_ref,
                 embed_ref, lse_ref, all_ref,
                 t_ref, tbuf, g_ref, gb0, gb1, c0, c1, rc0, rc1, key_ref, val_ref, self_ref, rcnt_ref, p_ref,
                 wm_ref, ws_ref, wn_ref, iota_ref, rows_own, rows_got, rows_sm, aux_own, aux, mail, near2, far2, logc_ref, stats, got, mine, final,
                 w_sem, in_sem, row_send, row_recv, aux_send, aux_recv, sm_sem, own_sem, q_send, q_recv,
                 send1, recv1, send2, recv2, load_sem, send3, recv3, send4, recv4):
    me = lax.axis_index("neg")
    q = lax.axis_index("qry")
    spot = (me // 4, lax.rem(me, 4))
    peers = [{"neg": lax.rem(me + d, 16)} for d in range(1, 16)]
    above, below = lax.rem(q + 2, 8), lax.rem(q + 6, 8)
    partner = q + 1 - 2 * lax.rem(q, 2)
    across = lax.rem(q + 4, 8)

    def device(axis, step):
        moved = lax.rem(spot[axis] + step + 4, 4)
        return {"neg": moved * 4 + spot[1] if axis == 0 else spot[0] * 4 + moved}

    weights = [
        pltpu.make_async_copy(source, target, w_sem.at[i])
        for i, (source, target) in enumerate(((wm_in, wm_ref), (ws_in, ws_ref), (wn_in, wn_ref)))
    ]
    for copy in weights:
        copy.start()
    iota_ref[...] = lax.broadcasted_iota(jnp.int32, (64, 128), 0)
    for j in range(16):
        rows_own[j] = fetch_ref[j:j + 1, :]
    count = count_ref[...]
    for h in range(2):
        ks = lax.broadcasted_iota(jnp.int32, (20, 512), 0) + 20 * h
        half = jnp.where(ks < count, slots_ref[20 * h:20 * h + 20, :], 0xFFFF)
        if h == 0:
            low = half
        else:
            aux_own[0:20, :] = low | jnp.left_shift(half, 16)
    aux_own[20:24, :] = jnp.broadcast_to(slot_ref[...] | jnp.left_shift(count, 16), (4, 512))

    sampled = sampled_ref[:, pl.ds(pl.multiple_of(q * 512, 128), 512)].astype(jnp.float32)
    logc_ref[...] = jnp.broadcast_to(jnp.log(sampled), (128, 512)).T

    row_peers = [{"qry": lax.rem(q + d, 8)} for d in range(1, 8)]
    greet(peers + row_peers)
    row_copies = []
    aux_copies = []
    for d, peer in enumerate(peers):
        other = lax.rem(me + d + 1, 16)
        row_copies.append(remote(rows_own.at[other], rows_got.at[me], row_send.at[d], row_recv.at[d], peer))
    for d, peer in enumerate(peers):
        aux_copies.append(remote(aux_own, aux.at[me], aux_send.at[d], aux_recv.at[d], peer))
    for copy in row_copies + aux_copies:
        copy.start()
    rows_got[me] = rows_own[me]
    aux[me] = aux_own[...]

    def pass_on(i, source, place, size, peer):
        return remote(source, all_ref.at[pl.ds(place, size)], q_send.at[i], q_recv.at[i], {"qry": peer})

    own_copy = pltpu.make_async_copy(queries_ref, all_ref.at[pl.ds(q * 2, 2)], own_sem)
    spread = [pass_on(i, queries_ref, q * 2, 2, peer) for i, peer in enumerate((above, below, partner))]

    def held(i, place, size, peer):
        return pass_on(i, all_ref.at[pl.ds(place, size)], place, size, peer)

    relay = [
        held(3, below * 2, 1, above),
        held(4, above * 2 + 1, 1, below),
        held(5, below * 2, 2, partner),
        held(6, above * 2, 2, partner),
    ]
    hand = [held(7, across * 2, 1, partner), held(8, across * 2 + 1, 1, partner)]
    own_copy.start()
    for copy in spread:
        copy.start()

    for copy in weights:
        copy.wait()
    build_table(table_ref, wm_ref, ws_ref, wn_ref, bm_ref, t_ref, tbuf, in_sem)

    for copy in row_copies:
        copy.wait_recv()
    to_scalar = [
        pltpu.make_async_copy(rows_got.at[j, 0], rows_sm.at[pl.ds(j * 640, 640)], sm_sem.at[j]) for j in range(16)
    ]
    for copy in to_scalar:
        copy.start()
    for copy in aux_copies:
        copy.wait_recv()
    last = aux[:, 20, :]
    last = jnp.concatenate([last] * 8, axis=0)
    self_ref[...] = (last & 0xFFFF).astype(jnp.float32).T
    rcnt_ref[...] = (1.0 / lax.shift_right_logical(last, 16).astype(jnp.float32)).T
    for copy in to_scalar:
        copy.wait()

    def near_copy(half, w, j):
        pair = (2, j) if half == 0 else (j, 2)
        rows = pl.ds(256 * half + 128 * w, 128)
        return remote(p_ref.at[PLACE[pair], rows, :], mail.at[half * 2 + w, j],
                      send1.at[half, w, 0, j], recv1.at[half, w, 0, j], device(half, 1 - 2 * w))

    def far_copy(half, w, stage, j):
        side = 1 + 2 * w
        pair = (side, j) if half == 0 else (j, side)
        part = w if stage == 2 else 1 - w
        rows = pl.ds(256 * half + 128 * part, 128)
        return remote(p_ref.at[PLACE[pair], rows, :], mail.at[4 + (half * 2 + w) * 2 + 2 - stage, j],
                      send1.at[half, w, stage, j], recv1.at[half, w, stage, j], device(half, 1 - 2 * w))

    def send_place(c):
        for half in range(2):
            d, j = ORDER[c][half], ORDER[c][1 - half]
            if d == 2:
                for w in range(2):
                    near_copy(half, w, j).start()
            elif d != 0:
                far_copy(half, (d - 1) // 2, 1, j).start()

    def step(dx, dy, gb, c, rc):
        n = lax.rem(spot[0] + dx, 4) * 4 + lax.rem(spot[1] + dy, 4)
        prepare(n, me, rows_sm, aux, t_ref, g_ref, self_ref, rcnt_ref, key_ref, val_ref, gb, c, rc, iota_ref)

    f32 = jnp.float32

    def carry(half, w, j):
        near_copy(half, w, j).wait_recv()
        side = 1 + 2 * w
        pair = (side, j) if half == 0 else (j, side)
        rows = slice(256 * half + 128 * w, 256 * half + 128 * w + 128)
        value = p_ref[PLACE[pair], rows, :].astype(f32) + mail[half * 2 + w, j].astype(f32)
        p_ref[PLACE[pair], rows, :] = value.astype(jnp.bfloat16)
        far_copy(half, w, 2, j).start()

    def home_at(half, j, part):
        first = 256 * half + 128 * part
        return PLACE[(0, j) if half == 0 else (j, 0)], slice(first, first + 128), slice(None)

    def second_copy(half, w, stage):
        target = (near2.at[half, w], far2.at[half, w, 1], far2.at[half, w, 0])[stage]
        place, rows, _ = home_at(half, (2, 1 + 2 * w, 1 + 2 * w)[stage], (w, 1 - w, w)[stage])
        return remote(p_ref.at[place, rows, :], target, send2.at[half, w, stage], recv2.at[half, w, stage],
                      device(1 - half, 1 - 2 * w))

    def arrive(half, j, part):
        far_copy(half, part, 2, j).wait_recv()
        far_copy(half, 1 - part, 1, j).wait_recv()

    def total(half, j, part):
        value = p_ref[home_at(half, j, part)].astype(f32) + mail[4 + (half * 2 + part) * 2, j].astype(f32)
        return value + mail[4 + (half * 2 + 1 - part) * 2 + 1, j].astype(f32)

    def home(half, j):
        for part in range(2):
            if j == 2 or part == 1 - (j - 1) // 2:
                arrive(half, j, part)
                p_ref[home_at(half, j, part)] = total(half, j, part).astype(jnp.bfloat16)
                if j == 2:
                    second_copy(half, part, 0).start()
                else:
                    second_copy(half, 1 - part, 1).start()

    def after(c):
        send_place(c)
        for (half, w, j), at in CARRY_AT.items():
            if at == c:
                carry(half, w, j)
        for (half, j), at in HOME_AT.items():
            if at == c:
                home(half, j)
        if c == RELAY_AT:
            for copy in spread:
                copy.wait_recv()
            for copy in relay:
                copy.start()
        if c == HAND_AT:
            for copy in relay:
                copy.wait_recv()
            for copy in hand:
                copy.start()

    step(ORDER[0][0], ORDER[0][1], gb0, c0, rc0)

    def two(i, codes):
        cx, cy = codes
        step(lax.rem(cx, 4), lax.rem(cy, 4), gb1, c1, rc1)
        p_ref[2 * i] = multiply(gb0, c0, rc0)
        for place in range(7):
            @pl.when(i == place)
            def _():
                after(2 * place)
        cx, cy = cx // 4, cy // 4
        step(lax.rem(cx, 4), lax.rem(cy, 4), gb0, c0, rc0)
        p_ref[2 * i + 1] = multiply(gb1, c1, rc1)
        for place in range(7):
            @pl.when(i == place)
            def _():
                after(2 * place + 1)
        return cx // 4, cy // 4
    lax.fori_loop(0, 7, two, (jnp.int32(CODE[0] // 4), jnp.int32(CODE[1] // 4)))
    step(ORDER[15][0], ORDER[15][1], gb1, c1, rc1)
    p_ref[14] = multiply(gb0, c0, rc0)
    after(14)
    p_ref[15] = multiply(gb1, c1, rc1)
    after(15)

    own_copy.wait()
    for copy in hand:
        copy.wait_recv()

    def load(i, slot):
        block = lax.rem(q + i + 1, 8)
        return pltpu.make_async_copy(all_ref.at[pl.ds(block * 2, 2)], mail.at[pl.ds(slot * 2, 2)], load_sem.at[slot])

    load(0, 0).start()
    load(1, 1).start()

    for half in range(2):
        for w in range(2):
            second_copy(half, w, 0).wait_recv()
            arrive(half, 1 + 2 * w, w)
            value = total(half, 1 + 2 * w, w) + near2[half, w].astype(f32)
            p_ref[home_at(half, 1 + 2 * w, w)] = value.astype(jnp.bfloat16)
            second_copy(half, w, 2).start()
    for half in range(2):
        for w in range(2):
            second_copy(half, w, 1).wait_recv()
            second_copy(half, w, 2).wait_recv()
        for w in range(2):
            rows = slice(256 * half + 128 * w, 256 * half + 128 * w + 128)
            arrive(half, 0, w)
            value = total(half, 0, w) + far2[half, w, 0].astype(f32) + far2[half, 1 - w, 1].astype(f32)
            hidden = jnp.maximum(value + bias_ref[...], 0.0)
            inv = lax.rsqrt(jnp.mean(hidden * hidden, axis=-1, keepdims=True) + 0.25)
            embed = (hidden * inv).astype(jnp.bfloat16)
            embed_ref[rows, :] = embed
            c0[rows, 0:512] = embed * jnp.bfloat16(0.25)
    for i in range(2, 6):
        load(i, i).start()

    def block_copy(d):
        return remote(stats.at[d - 1], got.at[q], send3.at[d - 1], recv3.at[d - 1], row_peers[d - 1])

    def block(i, _):
        slot = lax.rem(i, 6)
        load(i, slot).wait()
        for part in range(2):
            cols = pl.ds(part * 512, 512)
            scores = lax.dot_general(
                c0[:, 0:512], mail[2 * slot + part].reshape(512, 512), (((1,), (1,)), ((), ())),
                preferred_element_type=f32)
            scores = scores - jnp.concatenate([logc_ref[...]] * 4, axis=1)
            peak = jnp.max(scores, axis=0, keepdims=True)
            total = jnp.sum(jnp.exp(scores - peak), axis=0, keepdims=True)
            stats[i, 0:1, cols] = peak
            stats[i, 1:2, cols] = total
        for d in range(1, 8):
            @pl.when(i == d - 1)
            def _():
                block_copy(d).start()

        @pl.when(i < 2)
        def _():
            load(i + 6, slot).start()
        return 0
    lax.fori_loop(0, 8, block, 0)
    got[q] = stats[7]
    last_copies = [block_copy(d) for d in range(1, 8)]
    for copy in last_copies:
        copy.wait_recv()
    peak, total = joined(got[...])
    mine[...] = jnp.concatenate([peak, total], axis=0)
    final[me] = mine[...]
    for d, peer in enumerate(peers):
        last_copies.append(remote(mine, final.at[me], send4.at[d], recv4.at[d], peer))
        last_copies[-1].start()
    for copy in last_copies[7:]:
        copy.wait_recv()
    peak, total = joined(final[...])
    lse_ref[...] = peak + jnp.log(total) - math.log(65536)

    for copy in row_copies + aux_copies + spread + relay + hand + last_copies:
        copy.wait_send()
    for half in range(2):
        for w in range(2):
            for j in range(4):
                near_copy(half, w, j).wait_send()
                far_copy(half, w, 1, j).wait_send()
                far_copy(half, w, 2, j).wait_send()
            for stage in range(3):
                second_copy(half, w, stage).wait_send()


def joined(stats):
    peak = jnp.max(stats[:, 0:1, :], axis=0)
    total = jnp.sum(stats[:, 1:2, :] * jnp.exp(stats[:, 0:1, :] - peak[None]), axis=0)
    return peak, total


def tower(fetch_rows, slots, count, slot, table, wm, ws, wn, bm, bias, sampled, queries):
    any_space = pl.BlockSpec(memory_space=pl.ANY)
    bf16, f32, i32 = jnp.bfloat16, jnp.float32, jnp.int32
    dma = pltpu.SemaphoreType.DMA
    return pl.pallas_call(
        tower_kernel,
        out_shape=(
            jax.ShapeDtypeStruct((512, 512), bf16),
            jax.ShapeDtypeStruct((1, 1024), f32),
            jax.ShapeDtypeStruct((16, 4, 128, 512), bf16),
        ),
        in_specs=[VMEM] * 4 + [any_space] * 4 + [VMEM] * 3 + [any_space],
        out_specs=(VMEM, VMEM, any_space),
        scratch_shapes=[
            pltpu.VMEM((8192, 8, 128), f32),
            pltpu.VMEM((2, 512, 512), bf16),
            pltpu.VMEM((5768, 128), f32),
            pltpu.VMEM((640, 1024), bf16),
            pltpu.VMEM((640, 1024), bf16),
            pltpu.VMEM((512, 1280), bf16),
            pltpu.VMEM((512, 1280), bf16),
            pltpu.VMEM((512, 1), f32),
            pltpu.VMEM((512, 1), f32),
            pltpu.VMEM((48, 512), i32),
            pltpu.VMEM((48, 512), i32),
            pltpu.VMEM((512, 128), f32),
            pltpu.VMEM((512, 128), f32),
            pltpu.VMEM((16, 512, 512), bf16),
            pltpu.VMEM((512, 512), bf16),
            pltpu.VMEM((512, 512), bf16),
            pltpu.VMEM((512, 512), bf16),
            pltpu.VMEM((64, 128), i32),
            pltpu.VMEM((16, 1, 640), i32),
            pltpu.VMEM((16, 1, 640), i32),
            pltpu.SMEM((10240,), i32),
            pltpu.VMEM((24, 512), i32),
            pltpu.VMEM((16, 24, 512), i32),
            pltpu.VMEM((12, 4, 128, 512), bf16),
            pltpu.VMEM((2, 2, 128, 512), bf16),
            pltpu.VMEM((2, 2, 2, 128, 512), bf16),
            pltpu.VMEM((512, 128), f32),
            pltpu.VMEM((8, 2, 1024), f32),
            pltpu.VMEM((8, 2, 1024), f32),
            pltpu.VMEM((2, 1024), f32),
            pltpu.VMEM((16, 2, 1024), f32),
            dma((3,)), dma((2,)),
            dma((15,)), dma((15,)), dma((15,)), dma((15,)),
            dma((16,)), dma, dma((9,)), dma((9,)),
            dma((2, 2, 3, 4)), dma((2, 2, 3, 4)), dma((2, 2, 3)), dma((2, 2, 3)),
            dma((6,)), dma((7,)), dma((7,)), dma((15,)), dma((15,)),
        ],
        compiler_params=pltpu.CompilerParams(
            collective_id=1, has_side_effects=True, vmem_limit_bytes=67043328),
        name="tower",
    )(fetch_rows, slots, count, slot, table, wm, ws, wn, bm, bias, sampled, queries)


def per_device(
    items_table,
    fetch_rows,
    neighbour_slots,
    neighbour_count,
    self_slot,
    negative_count,
    message_weight,
    message_bias,
    self_weight,
    neighbour_weight,
    output_bias,
    queries,
):
    negative_embed, query_lse, _ = tower(
        fetch_rows, neighbour_slots.T, neighbour_count.reshape(1, 512), self_slot.reshape(1, 512), items_table,
        message_weight, self_weight, neighbour_weight, message_bias.reshape(1, 512), output_bias.reshape(1, 512),
        negative_count.reshape(1, 4096), queries.reshape(2, 4, 128, 512))
    return negative_embed, query_lse.reshape(1024)


def solution(mesh):
    in_specs = (
        P("neg", None),
        P(("neg", "qry"), None),
        P(("neg", "qry"), None),
        P(("neg", "qry")),
        P(("neg", "qry")),
        P("neg"),
        P(),
        P(),
        P(),
        P(),
        P(),
        P("qry", None),
    )
    out_specs = (P(("neg", "qry"), None), P("qry"))
    return jax.shard_map(
        per_device, mesh=mesh, in_specs=in_specs, out_specs=out_specs, check_vma=False
    )
```

```python
import functools
import math

import jax
import jax.numpy as jnp
from jax import lax
from jax.experimental import pallas as pl
from jax.experimental.pallas import tpu as pltpu
from jax.sharding import PartitionSpec as P

MESH = pl.DeviceIdType.MESH
VMEM = pl.BlockSpec(memory_space=pltpu.VMEM)


def remote(src, dst, send, recv, peer):
    return pltpu.make_async_remote_copy(
        src_ref=src, dst_ref=dst, send_sem=send, recv_sem=recv, device_id=peer, device_id_type=MESH
    )


def build_table(table_ref, wm_ref, ws_ref, wn_ref, bm_ref, t_ref, tbuf, spare, m_ref, in_sem):
    blk = 512
    flat = t_ref.reshape(65536, 128)

    def fetch(i, slot):
        target = tbuf.at[slot] if slot < 2 else spare.at[0:512, (slot - 2) * 512:(slot - 1) * 512]
        return pltpu.make_async_copy(table_ref.at[pl.ds(i * blk, blk), :], target, in_sem.at[slot])

    def dot(x, w_ref):
        return jnp.dot(x, w_ref[...], preferred_element_type=jnp.float32)

    def message(x):
        return jnp.maximum(dot(x, wm_ref) + bm_ref[...], 0.0).astype(jnp.bfloat16)

    def put(i, first, value):
        base = pl.multiple_of(i * (blk * 8), 8)
        for j in range(4):
            flat[pl.ds(base + first + j, blk, stride=8), :] = value[:, j * 128:(j + 1) * 128]


    def pair(i, slot, carried):
        fetch(2 * i, slot).wait()
        fetch(2 * i + 1, slot + 1).wait()
        if slot == 0:
            x, y = tbuf[0], tbuf[1]
        else:
            x, y = spare[0:512, 0:512], spare[0:512, 512:1024]
        if carried:
            before = m_ref[:, 0:512]
        mx = message(x)
        if carried:
            put(jnp.maximum(2 * i - 1, 0), 0, dot(before, wn_ref))
        put(2 * i, 4, dot(x, ws_ref))
        my = message(y)
        put(2 * i, 0, dot(mx, wn_ref))
        put(2 * i + 1, 4, dot(y, ws_ref))
        m_ref[:, 0:512] = my

    def build(i, _):
        fetch(4 * i + 2, 2).start()
        fetch(4 * i + 3, 3).start()
        pair(2 * i, 0, True)

        @pl.when(i < 3)
        def _():
            fetch(4 * i + 4, 0).start()
            fetch(4 * i + 5, 1).start()
        pair(2 * i + 1, 2, True)
        return 0
    m_ref[:, 0:512] = jnp.zeros((512, 512), jnp.bfloat16)
    lax.fori_loop(0, 4, build, 0)
    put(15, 0, dot(m_ref[:, 0:512], wn_ref))


GROUPS = ((0, 7), (7, 14), (14, 21), (21, 28), (28, 34), (34, 40))


def prepare(n, p, rows_ref, aux_ref, t_ref, g_ref, self_ref, rcnt_ref, key_ref, val_ref, gb_ref, c_ref, rc_ref, iota_ref):
    packed = aux_ref[n]
    for h, slots in enumerate((packed & 0xFFFF, lax.shift_right_logical(packed, 16))):
        rel = slots - 640 * p
        ok = (rel >= 0) & (rel < 640)
        key_ref[h * 24:(h + 1) * 24, :] = rel & 63
        shift = 3 * jnp.where(ok, lax.shift_right_logical(rel, 6), 0)
        val_ref[h * 24:(h + 1) * 24, :] = jnp.where(ok, jnp.left_shift(1, shift), 0)
    sub = lax.broadcasted_iota(jnp.int32, (64, 128), 0)
    lane = lax.broadcasted_iota(jnp.int32, (128, 128), 1)
    here = lane == n
    even = 0o0707070707
    for vb in range(4):
        for s in range(vb * 160, vb * 160 + 160):
            r = rows_ref[n * 640 + s]
            g_ref[s * 9:s * 9 + 8, :] = t_ref[r]
        cols = slice(vb * 128, (vb + 1) * 128)
        low = jnp.zeros((64, 128), jnp.int32)
        high = jnp.zeros((64, 128), jnp.int32)
        for first, last in GROUPS:
            acc = jnp.zeros((64, 128), jnp.int32)
            for k in range(first, last):
                kk = k if k < 20 else k + 4
                key = jnp.broadcast_to(key_ref[kk:kk + 1, cols], (64, 128))
                val = jnp.broadcast_to(val_ref[kk:kk + 1, cols], (64, 128))
                acc = acc + jnp.where(iota_ref[...] == key, val, 0)
            low = low + (acc & even)
            high = high + (lax.shift_right_logical(acc, 3) & even)
        ct = jnp.concatenate([low, high], axis=0).T
        self_col = jnp.sum(jnp.where(here, self_ref[cols, :], 0.0), axis=1, keepdims=True).astype(jnp.int32) - 640 * p
        rc_ref[cols, :] = jnp.sum(jnp.where(here, rcnt_ref[cols, :], 0.0), axis=1, keepdims=True)
        for f in range(5):
            c_ref[cols, f * 128:(f + 1) * 128] = (lax.shift_right_logical(ct, 6 * f) & 63).astype(jnp.float32).astype(jnp.bfloat16)
            c_ref[cols, 640 + f * 128:640 + (f + 1) * 128] = jnp.where(self_col == lane + f * 128, 1.0, 0.0).astype(jnp.bfloat16)
        for j in range(8):
            gb_ref[vb * 160:vb * 160 + 160, j * 128:(j + 1) * 128] = g_ref[pl.ds(vb * 1440 + j, 160, stride=9), :].astype(jnp.bfloat16)


def multiply(gb_ref, c_ref, rc_ref):
    part = jnp.dot(c_ref[:, :640], gb_ref[:, :512], preferred_element_type=jnp.float32) * rc_ref[...]
    part = part + jnp.dot(c_ref[:, 640:], gb_ref[:, 512:], preferred_element_type=jnp.float32)
    return part.astype(jnp.bfloat16)


ORDER = ((2, 2), (1, 2), (3, 2), (2, 1), (2, 3), (1, 1), (3, 3), (2, 0),
         (0, 2), (1, 3), (3, 1), (1, 0), (0, 1), (3, 0), (0, 3), (0, 0))
PLACE = {pair: i for i, pair in enumerate(ORDER)}
CODE = tuple(sum(pair[axis] * 4 ** i for i, pair in enumerate(ORDER)) for axis in range(2))


CARRY_AT = {
    (0, 0, 2): 3, (0, 1, 2): 3, (1, 0, 2): 4, (1, 1, 2): 4, (0, 0, 1): 7, (0, 1, 1): 10, (0, 0, 3): 9, (0, 1, 3): 8,
    (1, 0, 1): 6, (1, 1, 1): 9, (1, 0, 3): 10, (1, 1, 3): 7, (0, 0, 0): 11, (0, 1, 0): 13, (1, 0, 0): 12, (1, 1, 0): 14,
}
HOME_AT = {(0, 2): 8, (1, 2): 9, (1, 1): 13, (0, 1): 15, (0, 3): 15, (1, 3): 15}
RELAY_AT, HAND_AT = 5, 12

def tower_kernel(fetch_ref, slots_ref, count_ref, slot_ref, table_ref, wm_in, ws_in, wn_in, bm_ref, bias_ref,
                 sampled_ref, queries_ref,
                 embed_ref, lse_ref, all_ref,
                 t_ref, tbuf, g_ref, gb0, gb1, c0, c1, rc0, rc1, key_ref, val_ref, self_ref, rcnt_ref, p_ref,
                 wm_ref, ws_ref, wn_ref, iota_ref, rows_own, rows_got, rows_sm, aux_own, aux, mail, near2, far2, logc_ref, stats, got, mine, final,
                 w_sem, in_sem, row_send, row_recv, aux_send, aux_recv, sm_sem, own_sem, q_send, q_recv,
                 send1, recv1, send2, recv2, load_sem, send3, recv3, send4, recv4):
    me = lax.axis_index("neg")
    q = lax.axis_index("qry")
    spot = (me // 4, lax.rem(me, 4))
    peers = [{"neg": lax.rem(me + d, 16)} for d in range(1, 16)]
    above, below = lax.rem(q + 2, 8), lax.rem(q + 6, 8)
    partner = q + 1 - 2 * lax.rem(q, 2)
    across = lax.rem(q + 4, 8)

    def device(axis, step):
        moved = lax.rem(spot[axis] + step + 4, 4)
        return {"neg": moved * 4 + spot[1] if axis == 0 else spot[0] * 4 + moved}

    weights = [
        pltpu.make_async_copy(source, target, w_sem.at[i])
        for i, (source, target) in enumerate(((wm_in, wm_ref), (ws_in, ws_ref), (wn_in, wn_ref)))
    ]
    for copy in weights:
        copy.start()
    for i in range(2):
        pltpu.make_async_copy(table_ref.at[pl.ds(i * 512, 512), :], tbuf.at[i], in_sem.at[i]).start()
    row_peers = [{"qry": lax.rem(q + d, 8)} for d in range(1, 8)]
    barrier = pltpu.get_barrier_semaphore()
    for peer in peers + row_peers:
        pl.semaphore_signal(barrier, inc=1, device_id=peer, device_id_type=MESH)
    iota_ref[...] = lax.broadcasted_iota(jnp.int32, (64, 128), 0)
    for j in range(16):
        rows_own[j] = fetch_ref[j:j + 1, :]
    count = count_ref[...]
    for h in range(2):
        ks = lax.broadcasted_iota(jnp.int32, (20, 512), 0) + 20 * h
        half = jnp.where(ks < count, slots_ref[20 * h:20 * h + 20, :], 0xFFFF)
        if h == 0:
            low = half
        else:
            aux_own[0:20, :] = low | jnp.left_shift(half, 16)
    aux_own[20:24, :] = jnp.broadcast_to(slot_ref[...] | jnp.left_shift(count, 16), (4, 512))

    pl.semaphore_wait(barrier, len(peers + row_peers))
    row_copies = []
    aux_copies = []
    for d, peer in enumerate(peers):
        other = lax.rem(me + d + 1, 16)
        row_copies.append(remote(rows_own.at[other], rows_got.at[me], row_send.at[d], row_recv.at[d], peer))
    for d, peer in enumerate(peers):
        aux_copies.append(remote(aux_own, aux.at[me], aux_send.at[d], aux_recv.at[d], peer))
    for copy in row_copies + aux_copies:
        copy.start()
    rows_got[me] = rows_own[me]
    aux[me] = aux_own[...]

    def pass_on(i, source, place, size, peer):
        return remote(source, all_ref.at[pl.ds(place, size)], q_send.at[i], q_recv.at[i], {"qry": peer})

    own_copy = pltpu.make_async_copy(queries_ref, all_ref.at[pl.ds(q * 2, 2)], own_sem)
    spread = [pass_on(i, queries_ref, q * 2, 2, peer) for i, peer in enumerate((above, below, partner))]

    def held(i, place, size, peer):
        return pass_on(i, all_ref.at[pl.ds(place, size)], place, size, peer)

    relay = [
        held(3, below * 2, 1, above),
        held(4, above * 2 + 1, 1, below),
        held(5, below * 2, 2, partner),
        held(6, above * 2, 2, partner),
    ]
    hand = [held(7, across * 2, 1, partner), held(8, across * 2 + 1, 1, partner)]
    own_copy.start()
    for copy in spread:
        copy.start()

    sampled = sampled_ref[:, pl.ds(pl.multiple_of(q * 512, 128), 512)].astype(jnp.float32)
    logc_ref[...] = jnp.broadcast_to(jnp.log(sampled), (128, 512)).T

    for copy in weights:
        copy.wait()
    build_table(table_ref, wm_ref, ws_ref, wn_ref, bm_ref, t_ref, tbuf, gb1, c0, in_sem)

    for copy in row_copies:
        copy.wait_recv()
    to_scalar = [
        pltpu.make_async_copy(rows_got.at[j, 0], rows_sm.at[pl.ds(j * 640, 640)], sm_sem.at[j]) for j in range(16)
    ]
    for copy in to_scalar:
        copy.start()
    for copy in aux_copies:
        copy.wait_recv()
    last = aux[:, 20, :]
    last = jnp.concatenate([last] * 8, axis=0)
    self_ref[...] = (last & 0xFFFF).astype(jnp.float32).T
    rcnt_ref[...] = (1.0 / lax.shift_right_logical(last, 16).astype(jnp.float32)).T
    for copy in to_scalar:
        copy.wait()

    def near_copy(half, w, j):
        pair = (2, j) if half == 0 else (j, 2)
        rows = pl.ds(256 * half + 128 * w, 128)
        return remote(p_ref.at[PLACE[pair], rows, :], mail.at[half * 2 + w, j],
                      send1.at[half, w, 0, j], recv1.at[half, w, 0, j], device(half, 1 - 2 * w))

    def far_copy(half, w, stage, j):
        side = 1 + 2 * w
        pair = (side, j) if half == 0 else (j, side)
        part = w if stage == 2 else 1 - w
        rows = pl.ds(256 * half + 128 * part, 128)
        return remote(p_ref.at[PLACE[pair], rows, :], mail.at[4 + (half * 2 + w) * 2 + 2 - stage, j],
                      send1.at[half, w, stage, j], recv1.at[half, w, stage, j], device(half, 1 - 2 * w))

    def send_place(c):
        for half in range(2):
            d, j = ORDER[c][half], ORDER[c][1 - half]
            if d == 2:
                for w in range(2):
                    near_copy(half, w, j).start()
            elif d != 0:
                far_copy(half, (d - 1) // 2, 1, j).start()

    def step(dx, dy, gb, c, rc):
        n = lax.rem(spot[0] + dx, 4) * 4 + lax.rem(spot[1] + dy, 4)
        prepare(n, me, rows_sm, aux, t_ref, g_ref, self_ref, rcnt_ref, key_ref, val_ref, gb, c, rc, iota_ref)

    f32 = jnp.float32

    def carry(half, w, j):
        near_copy(half, w, j).wait_recv()
        side = 1 + 2 * w
        pair = (side, j) if half == 0 else (j, side)
        rows = slice(256 * half + 128 * w, 256 * half + 128 * w + 128)
        value = p_ref[PLACE[pair], rows, :].astype(f32) + mail[half * 2 + w, j].astype(f32)
        p_ref[PLACE[pair], rows, :] = value.astype(jnp.bfloat16)
        far_copy(half, w, 2, j).start()

    def home_at(half, j, part):
        first = 256 * half + 128 * part
        return PLACE[(0, j) if half == 0 else (j, 0)], slice(first, first + 128), slice(None)

    def second_copy(half, w, stage):
        target = (near2.at[half, w], far2.at[half, w, 1], far2.at[half, w, 0])[stage]
        place, rows, _ = home_at(half, (2, 1 + 2 * w, 1 + 2 * w)[stage], (w, 1 - w, w)[stage])
        return remote(p_ref.at[place, rows, :], target, send2.at[half, w, stage], recv2.at[half, w, stage],
                      device(1 - half, 1 - 2 * w))

    def arrive(half, j, part):
        far_copy(half, part, 2, j).wait_recv()
        far_copy(half, 1 - part, 1, j).wait_recv()

    def total(half, j, part):
        value = p_ref[home_at(half, j, part)].astype(f32) + mail[4 + (half * 2 + part) * 2, j].astype(f32)
        return value + mail[4 + (half * 2 + 1 - part) * 2 + 1, j].astype(f32)

    def home(half, j):
        for part in range(2):
            if j == 2 or part == 1 - (j - 1) // 2:
                arrive(half, j, part)
                p_ref[home_at(half, j, part)] = total(half, j, part).astype(jnp.bfloat16)
                if j == 2:
                    second_copy(half, part, 0).start()
                else:
                    second_copy(half, 1 - part, 1).start()

    def after(c):
        send_place(c)
        for (half, w, j), at in CARRY_AT.items():
            if at == c:
                carry(half, w, j)
        for (half, j), at in HOME_AT.items():
            if at == c:
                home(half, j)
        if c == RELAY_AT:
            for copy in spread:
                copy.wait_recv()
            for copy in relay:
                copy.start()
        if c == HAND_AT:
            for copy in relay:
                copy.wait_recv()
            for copy in hand:
                copy.start()

    step(ORDER[0][0], ORDER[0][1], gb0, c0, rc0)

    def two(i, codes):
        cx, cy = codes
        step(lax.rem(cx, 4), lax.rem(cy, 4), gb1, c1, rc1)
        p_ref[2 * i] = multiply(gb0, c0, rc0)
        for place in range(7):
            @pl.when(i == place)
            def _():
                after(2 * place)
        cx, cy = cx // 4, cy // 4
        step(lax.rem(cx, 4), lax.rem(cy, 4), gb0, c0, rc0)
        p_ref[2 * i + 1] = multiply(gb1, c1, rc1)
        for place in range(7):
            @pl.when(i == place)
            def _():
                after(2 * place + 1)
        return cx // 4, cy // 4
    lax.fori_loop(0, 7, two, (jnp.int32(CODE[0] // 4), jnp.int32(CODE[1] // 4)))
    step(ORDER[15][0], ORDER[15][1], gb1, c1, rc1)
    p_ref[14] = multiply(gb0, c0, rc0)
    after(14)
    p_ref[15] = multiply(gb1, c1, rc1)
    after(15)

    own_copy.wait()
    for copy in hand:
        copy.wait_recv()

    def load(i, slot):
        block = lax.rem(q + i + 1, 8)
        return pltpu.make_async_copy(all_ref.at[pl.ds(block * 2, 2)], mail.at[pl.ds(slot * 2, 2)], load_sem.at[slot])

    load(0, 0).start()
    load(1, 1).start()

    for half in range(2):
        for w in range(2):
            second_copy(half, w, 0).wait_recv()
            arrive(half, 1 + 2 * w, w)
            value = total(half, 1 + 2 * w, w) + near2[half, w].astype(f32)
            p_ref[home_at(half, 1 + 2 * w, w)] = value.astype(jnp.bfloat16)
            second_copy(half, w, 2).start()
    for half in range(2):
        for w in range(2):
            second_copy(half, w, 1).wait_recv()
            second_copy(half, w, 2).wait_recv()
        for w in range(2):
            rows = slice(256 * half + 128 * w, 256 * half + 128 * w + 128)
            arrive(half, 0, w)
            value = total(half, 0, w) + far2[half, w, 0].astype(f32) + far2[half, 1 - w, 1].astype(f32)
            hidden = jnp.maximum(value + bias_ref[...], 0.0)
            inv = lax.rsqrt(jnp.mean(hidden * hidden, axis=-1, keepdims=True) + 0.25)
            embed = (hidden * inv).astype(jnp.bfloat16)
            embed_ref[rows, :] = embed
            c0[rows, 0:512] = embed * jnp.bfloat16(0.25)
    for i in range(2, 6):
        load(i, i).start()

    def block_copy(d):
        return remote(stats.at[d - 1], got.at[q], send3.at[d - 1], recv3.at[d - 1], row_peers[d - 1])

    def block(i, _):
        slot = lax.rem(i, 6)
        load(i, slot).wait()
        for part in range(2):
            cols = pl.ds(part * 512, 512)
            scores = lax.dot_general(
                c0[:, 0:512], mail[2 * slot + part].reshape(512, 512), (((1,), (1,)), ((), ())),
                preferred_element_type=f32)
            scores = scores - jnp.concatenate([logc_ref[...]] * 4, axis=1)
            peak = jnp.max(scores, axis=0, keepdims=True)
            total = jnp.sum(jnp.exp(scores - peak), axis=0, keepdims=True)
            stats[i, 0:1, cols] = peak
            stats[i, 1:2, cols] = total
        for d in range(1, 8):
            @pl.when(i == d - 1)
            def _():
                block_copy(d).start()

        @pl.when(i < 2)
        def _():
            load(i + 6, slot).start()
        return 0
    lax.fori_loop(0, 8, block, 0)
    got[q] = stats[7]
    last_copies = [block_copy(d) for d in range(1, 8)]
    for copy in last_copies:
        copy.wait_recv()
    peak, total = joined(got[...])
    mine[...] = jnp.concatenate([peak, total], axis=0)
    final[me] = mine[...]
    for d, peer in enumerate(peers):
        last_copies.append(remote(mine, final.at[me], send4.at[d], recv4.at[d], peer))
        last_copies[-1].start()
    for copy in last_copies[7:]:
        copy.wait_recv()
    peak, total = joined(final[...])
    lse_ref[...] = peak + jnp.log(total) - math.log(65536)

    for copy in row_copies + aux_copies + spread + relay + hand + last_copies:
        copy.wait_send()
    for half in range(2):
        for w in range(2):
            for j in range(4):
                near_copy(half, w, j).wait_send()
                far_copy(half, w, 1, j).wait_send()
                far_copy(half, w, 2, j).wait_send()
            for stage in range(3):
                second_copy(half, w, stage).wait_send()


def joined(stats):
    peak = jnp.max(stats[:, 0:1, :], axis=0)
    total = jnp.sum(stats[:, 1:2, :] * jnp.exp(stats[:, 0:1, :] - peak[None]), axis=0)
    return peak, total


def tower(fetch_rows, slots, count, slot, table, wm, ws, wn, bm, bias, sampled, queries):
    any_space = pl.BlockSpec(memory_space=pl.ANY)
    bf16, f32, i32 = jnp.bfloat16, jnp.float32, jnp.int32
    dma = pltpu.SemaphoreType.DMA
    return pl.pallas_call(
        tower_kernel,
        out_shape=(
            jax.ShapeDtypeStruct((512, 512), bf16),
            jax.ShapeDtypeStruct((1, 1024), f32),
            jax.ShapeDtypeStruct((16, 4, 128, 512), bf16),
        ),
        in_specs=[VMEM] * 4 + [any_space] * 4 + [VMEM] * 3 + [any_space],
        out_specs=(VMEM, VMEM, any_space),
        scratch_shapes=[
            pltpu.VMEM((8192, 8, 128), f32),
            pltpu.VMEM((2, 512, 512), bf16),
            pltpu.VMEM((5768, 128), f32),
            pltpu.VMEM((640, 1024), bf16),
            pltpu.VMEM((640, 1024), bf16),
            pltpu.VMEM((512, 1280), bf16),
            pltpu.VMEM((512, 1280), bf16),
            pltpu.VMEM((512, 1), f32),
            pltpu.VMEM((512, 1), f32),
            pltpu.VMEM((48, 512), i32),
            pltpu.VMEM((48, 512), i32),
            pltpu.VMEM((512, 128), f32),
            pltpu.VMEM((512, 128), f32),
            pltpu.VMEM((16, 512, 512), bf16),
            pltpu.VMEM((512, 512), bf16),
            pltpu.VMEM((512, 512), bf16),
            pltpu.VMEM((512, 512), bf16),
            pltpu.VMEM((64, 128), i32),
            pltpu.VMEM((16, 1, 640), i32),
            pltpu.VMEM((16, 1, 640), i32),
            pltpu.SMEM((10240,), i32),
            pltpu.VMEM((24, 512), i32),
            pltpu.VMEM((16, 24, 512), i32),
            pltpu.VMEM((12, 4, 128, 512), bf16),
            pltpu.VMEM((2, 2, 128, 512), bf16),
            pltpu.VMEM((2, 2, 2, 128, 512), bf16),
            pltpu.VMEM((512, 128), f32),
            pltpu.VMEM((8, 2, 1024), f32),
            pltpu.VMEM((8, 2, 1024), f32),
            pltpu.VMEM((2, 1024), f32),
            pltpu.VMEM((16, 2, 1024), f32),
            dma((3,)), dma((4,)),
            dma((15,)), dma((15,)), dma((15,)), dma((15,)),
            dma((16,)), dma, dma((9,)), dma((9,)),
            dma((2, 2, 3, 4)), dma((2, 2, 3, 4)), dma((2, 2, 3)), dma((2, 2, 3)),
            dma((6,)), dma((7,)), dma((7,)), dma((15,)), dma((15,)),
        ],
        compiler_params=pltpu.CompilerParams(
            collective_id=1, has_side_effects=True, vmem_limit_bytes=67043328),
        name="tower",
    )(fetch_rows, slots, count, slot, table, wm, ws, wn, bm, bias, sampled, queries)


def per_device(
    items_table,
    fetch_rows,
    neighbour_slots,
    neighbour_count,
    self_slot,
    negative_count,
    message_weight,
    message_bias,
    self_weight,
    neighbour_weight,
    output_bias,
    queries,
):
    negative_embed, query_lse, _ = tower(
        fetch_rows, neighbour_slots.T, neighbour_count.reshape(1, 512), self_slot.reshape(1, 512), items_table,
        message_weight, self_weight, neighbour_weight, message_bias.reshape(1, 512), output_bias.reshape(1, 512),
        negative_count.reshape(1, 4096), queries.reshape(2, 4, 128, 512))
    return negative_embed, query_lse.reshape(1024)


def solution(mesh):
    in_specs = (
        P("neg", None),
        P(("neg", "qry"), None),
        P(("neg", "qry"), None),
        P(("neg", "qry")),
        P(("neg", "qry")),
        P("neg"),
        P(),
        P(),
        P(),
        P(),
        P(),
        P("qry", None),
    )
    out_specs = (P(("neg", "qry"), None), P("qry"))
    return jax.shard_map(
        per_device, mesh=mesh, in_specs=in_specs, out_specs=out_specs, check_vma=False
    )
```

```python
import functools
import math

import jax
import jax.numpy as jnp
from jax import lax
from jax.experimental import pallas as pl
from jax.experimental.pallas import tpu as pltpu
from jax.sharding import PartitionSpec as P

MESH = pl.DeviceIdType.MESH
VMEM = pl.BlockSpec(memory_space=pltpu.VMEM)


def remote(src, dst, send, recv, peer):
    return pltpu.make_async_remote_copy(
        src_ref=src, dst_ref=dst, send_sem=send, recv_sem=recv, device_id=peer, device_id_type=MESH
    )


def build_table(table_ref, wm_ref, ws_ref, wn_ref, bm_ref, t_ref, tbuf, spare, m_ref, in_sem):
    blk = 512
    flat = t_ref.reshape(65536, 128)

    def fetch(i, slot):
        target = tbuf.at[slot] if slot < 2 else spare.at[0:512, (slot - 2) * 512:(slot - 1) * 512]
        return pltpu.make_async_copy(table_ref.at[pl.ds(i * blk, blk), :], target, in_sem.at[slot])

    def dot(x, w_ref):
        return jnp.dot(x, w_ref[...], preferred_element_type=jnp.float32)

    def message(x):
        return jnp.maximum(dot(x, wm_ref) + bm_ref[...], 0.0).astype(jnp.bfloat16)

    def put(i, first, value):
        base = pl.multiple_of(i * (blk * 8), 8)
        for j in range(4):
            flat[pl.ds(base + first + j, blk, stride=8), :] = value[:, j * 128:(j + 1) * 128]


    def pair(i, slot, carried):
        fetch(2 * i, slot).wait()
        fetch(2 * i + 1, slot + 1).wait()
        if slot == 0:
            x, y = tbuf[0], tbuf[1]
        else:
            x, y = spare[0:512, 0:512], spare[0:512, 512:1024]
        if carried:
            before = m_ref[:, 0:512]
        mx = message(x)
        if carried:
            put(jnp.maximum(2 * i - 1, 0), 0, dot(before, wn_ref))
        put(2 * i, 4, dot(x, ws_ref))
        my = message(y)
        put(2 * i, 0, dot(mx, wn_ref))
        put(2 * i + 1, 4, dot(y, ws_ref))
        m_ref[:, 0:512] = my

    def build(i, _):
        fetch(4 * i + 2, 2).start()
        fetch(4 * i + 3, 3).start()
        pair(2 * i, 0, True)

        @pl.when(i < 3)
        def _():
            fetch(4 * i + 4, 0).start()
            fetch(4 * i + 5, 1).start()
        pair(2 * i + 1, 2, True)
        return 0
    m_ref[:, 0:512] = jnp.zeros((512, 512), jnp.bfloat16)
    lax.fori_loop(0, 4, build, 0)
    put(15, 0, dot(m_ref[:, 0:512], wn_ref))


GROUPS = ((0, 7), (7, 14), (14, 21), (21, 28), (28, 34), (34, 40))


def prepare(n, p, rows_ref, aux_ref, t_ref, g_ref, self_ref, rcnt_ref, key_ref, val_ref, gb_ref, c_ref, rc_ref, iota_ref):
    packed = aux_ref[n]
    for h, slots in enumerate((packed & 0xFFFF, lax.shift_right_logical(packed, 16))):
        rel = slots - 640 * p
        ok = (rel >= 0) & (rel < 640)
        key_ref[h * 24:(h + 1) * 24, :] = rel & 63
        shift = 3 * jnp.where(ok, lax.shift_right_logical(rel, 6), 0)
        val_ref[h * 24:(h + 1) * 24, :] = jnp.where(ok, jnp.left_shift(1, shift), 0)
    sub = lax.broadcasted_iota(jnp.int32, (64, 128), 0)
    lane = lax.broadcasted_iota(jnp.int32, (128, 128), 1)
    here = lane == n
    even = 0o0707070707
    for vb in range(4):
        for s in range(vb * 160, vb * 160 + 160):
            r = rows_ref[n * 640 + s]
            g_ref[s * 9:s * 9 + 8, :] = t_ref[r]
        cols = slice(vb * 128, (vb + 1) * 128)
        low = jnp.zeros((64, 128), jnp.int32)
        high = jnp.zeros((64, 128), jnp.int32)
        for first, last in GROUPS:
            acc = jnp.zeros((64, 128), jnp.int32)
            for k in range(first, last):
                kk = k if k < 20 else k + 4
                key = jnp.broadcast_to(key_ref[kk:kk + 1, cols], (64, 128))
                val = jnp.broadcast_to(val_ref[kk:kk + 1, cols], (64, 128))
                acc = acc + jnp.where(iota_ref[...] == key, val, 0)
            low = low + (acc & even)
            high = high + (lax.shift_right_logical(acc, 3) & even)
        ct = jnp.concatenate([low, high], axis=0).T
        self_col = jnp.sum(jnp.where(here, self_ref[cols, :], 0.0), axis=1, keepdims=True).astype(jnp.int32) - 640 * p
        rc_ref[cols, :] = jnp.sum(jnp.where(here, rcnt_ref[cols, :], 0.0), axis=1, keepdims=True)
        for f in range(5):
            c_ref[cols, f * 128:(f + 1) * 128] = (lax.shift_right_logical(ct, 6 * f) & 63).astype(jnp.float32).astype(jnp.bfloat16)
            c_ref[cols, 640 + f * 128:640 + (f + 1) * 128] = jnp.where(self_col == lane + f * 128, 1.0, 0.0).astype(jnp.bfloat16)
        for j in range(8):
            gb_ref[vb * 160:vb * 160 + 160, j * 128:(j + 1) * 128] = g_ref[pl.ds(vb * 1440 + j, 160, stride=9), :].astype(jnp.bfloat16)


def multiply(gb_ref, c_ref, rc_ref):
    part = jnp.dot(c_ref[:, :640], gb_ref[:, :512], preferred_element_type=jnp.float32) * rc_ref[...]
    part = part + jnp.dot(c_ref[:, 640:], gb_ref[:, 512:], preferred_element_type=jnp.float32)
    return part.astype(jnp.bfloat16)


ORDER = ((2, 2), (1, 2), (3, 2), (2, 1), (2, 3), (1, 1), (3, 3), (2, 0),
         (0, 2), (1, 3), (3, 1), (1, 0), (0, 1), (3, 0), (0, 3), (0, 0))
PLACE = {pair: i for i, pair in enumerate(ORDER)}
CODE = tuple(sum(pair[axis] * 4 ** i for i, pair in enumerate(ORDER)) for axis in range(2))


CARRY_AT = {
    (0, 0, 2): 3, (0, 1, 2): 3, (1, 0, 2): 4, (1, 1, 2): 4, (0, 0, 1): 7, (0, 1, 1): 10, (0, 0, 3): 9, (0, 1, 3): 8,
    (1, 0, 1): 6, (1, 1, 1): 9, (1, 0, 3): 10, (1, 1, 3): 7, (0, 0, 0): 11, (0, 1, 0): 13, (1, 0, 0): 12, (1, 1, 0): 14,
}
HOME_AT = {(0, 2): 8, (1, 2): 9, (1, 1): 13, (0, 1): 15, (0, 3): 15, (1, 3): 15}
RELAY_AT, HAND_AT = 5, 12

def tower_kernel(fetch_ref, slots_ref, count_ref, slot_ref, table_ref, wm_in, ws_in, wn_in, bm_ref, bias_ref,
                 sampled_ref, queries_ref,
                 embed_ref, lse_ref, all_ref,
                 t_ref, tbuf, g_ref, gb0, gb1, c0, c1, rc0, rc1, key_ref, val_ref, self_ref, rcnt_ref, p_ref,
                 wm_ref, ws_ref, wn_ref, iota_ref, rows_own, rows_got, rows_sm, aux_own, aux, mail, near2, far2, logc_ref, stats, got, mine, final,
                 w_sem, in_sem, row_send, row_recv, aux_send, aux_recv, sm_sem, own_sem, q_send, q_recv,
                 send1, recv1, send2, recv2, load_sem, send3, recv3, send4, recv4):
    me = lax.axis_index("neg")
    q = lax.axis_index("qry")
    spot = (me // 4, lax.rem(me, 4))
    peers = [{"neg": lax.rem(me + d, 16)} for d in range(1, 16)]
    above, below = lax.rem(q + 2, 8), lax.rem(q + 6, 8)
    partner = q + 1 - 2 * lax.rem(q, 2)
    across = lax.rem(q + 4, 8)

    def device(axis, step):
        moved = lax.rem(spot[axis] + step + 4, 4)
        return {"neg": moved * 4 + spot[1] if axis == 0 else spot[0] * 4 + moved}

    weights = [
        pltpu.make_async_copy(source, target, w_sem.at[i])
        for i, (source, target) in enumerate(((wm_in, wm_ref), (ws_in, ws_ref), (wn_in, wn_ref)))
    ]
    for copy in weights:
        copy.start()
    for i in range(2):
        pltpu.make_async_copy(table_ref.at[pl.ds(i * 512, 512), :], tbuf.at[i], in_sem.at[i]).start()
    row_peers = [{"qry": lax.rem(q + d, 8)} for d in range(1, 8)]
    barrier = pltpu.get_barrier_semaphore()
    for peer in peers + row_peers:
        pl.semaphore_signal(barrier, inc=1, device_id=peer, device_id_type=MESH)
    iota_ref[...] = lax.broadcasted_iota(jnp.int32, (64, 128), 0)
    for j in range(16):
        rows_own[j] = fetch_ref[j:j + 1, :]
    count = count_ref[...]
    for h in range(2):
        ks = lax.broadcasted_iota(jnp.int32, (20, 512), 0) + 20 * h
        half = jnp.where(ks < count, slots_ref[20 * h:20 * h + 20, :], 0xFFFF)
        if h == 0:
            low = half
        else:
            aux_own[0:20, :] = low | jnp.left_shift(half, 16)
    aux_own[20:24, :] = jnp.broadcast_to(slot_ref[...] | jnp.left_shift(count, 16), (4, 512))

    pl.semaphore_wait(barrier, len(peers + row_peers))
    row_copies = []
    aux_copies = []
    for d, peer in enumerate(peers):
        other = lax.rem(me + d + 1, 16)
        row_copies.append(remote(rows_own.at[other], rows_got.at[me], row_send.at[d], row_recv.at[d], peer))
    for d, peer in enumerate(peers):
        aux_copies.append(remote(aux_own, aux.at[me], aux_send.at[d], aux_recv.at[d], peer))
    for copy in row_copies + aux_copies:
        copy.start()
    rows_got[me] = rows_own[me]
    aux[me] = aux_own[...]

    def pass_on(i, source, place, size, peer):
        return remote(source, all_ref.at[pl.ds(place, size)], q_send.at[i], q_recv.at[i], {"qry": peer})

    own_copy = pltpu.make_async_copy(queries_ref, all_ref.at[pl.ds(q * 2, 2)], own_sem)
    spread = [pass_on(i, queries_ref, q * 2, 2, peer) for i, peer in enumerate((above, below, partner))]

    def held(i, place, size, peer):
        return pass_on(i, all_ref.at[pl.ds(place, size)], place, size, peer)

    relay = [
        held(3, below * 2, 1, above),
        held(4, above * 2 + 1, 1, below),
        held(5, below * 2, 2, partner),
        held(6, above * 2, 2, partner),
    ]
    hand = [held(7, across * 2, 1, partner), held(8, across * 2 + 1, 1, partner)]
    own_copy.start()
    for copy in spread:
        copy.start()

    sampled = sampled_ref[:, pl.ds(pl.multiple_of(q * 512, 128), 512)].astype(jnp.float32)
    logc_ref[...] = jnp.broadcast_to(jnp.log(sampled), (128, 512)).T

    for copy in weights:
        copy.wait()
    build_table(table_ref, wm_ref, ws_ref, wn_ref, bm_ref, t_ref, tbuf, gb1, c0, in_sem)

    for copy in row_copies:
        copy.wait_recv()
    to_scalar = [
        pltpu.make_async_copy(rows_got.at[j, 0], rows_sm.at[pl.ds(j * 640, 640)], sm_sem.at[j]) for j in range(16)
    ]
    for copy in to_scalar:
        copy.start()
    for copy in aux_copies:
        copy.wait_recv()
    last = aux[:, 20, :]
    last = jnp.concatenate([last] * 8, axis=0)
    self_ref[...] = (last & 0xFFFF).astype(jnp.float32).T
    rcnt_ref[...] = (1.0 / lax.shift_right_logical(last, 16).astype(jnp.float32)).T
    for copy in to_scalar:
        copy.wait()

    def near_copy(half, w, j):
        pair = (2, j) if half == 0 else (j, 2)
        rows = pl.ds(256 * half + 128 * w, 128)
        return remote(p_ref.at[PLACE[pair], rows, :], mail.at[half * 2 + w, j],
                      send1.at[half, w, 0, j], recv1.at[half, w, 0, j], device(half, 1 - 2 * w))

    def far_copy(half, w, stage, j):
        side = 1 + 2 * w
        pair = (side, j) if half == 0 else (j, side)
        part = w if stage == 2 else 1 - w
        rows = pl.ds(256 * half + 128 * part, 128)
        return remote(p_ref.at[PLACE[pair], rows, :], mail.at[4 + (half * 2 + w) * 2 + 2 - stage, j],
                      send1.at[half, w, stage, j], recv1.at[half, w, stage, j], device(half, 1 - 2 * w))

    def send_place(c):
        for half in range(2):
            d, j = ORDER[c][half], ORDER[c][1 - half]
            if d == 2:
                for w in range(2):
                    near_copy(half, w, j).start()
            elif d != 0:
                far_copy(half, (d - 1) // 2, 1, j).start()

    def step(dx, dy, gb, c, rc):
        n = lax.rem(spot[0] + dx, 4) * 4 + lax.rem(spot[1] + dy, 4)
        prepare(n, me, rows_sm, aux, t_ref, g_ref, self_ref, rcnt_ref, key_ref, val_ref, gb, c, rc, iota_ref)

    f32 = jnp.float32

    def carry(half, w, j):
        near_copy(half, w, j).wait_recv()
        side = 1 + 2 * w
        pair = (side, j) if half == 0 else (j, side)
        rows = slice(256 * half + 128 * w, 256 * half + 128 * w + 128)
        value = p_ref[PLACE[pair], rows, :].astype(f32) + mail[half * 2 + w, j].astype(f32)
        p_ref[PLACE[pair], rows, :] = value.astype(jnp.bfloat16)
        far_copy(half, w, 2, j).start()

    def home_at(half, j, part):
        first = 256 * half + 128 * part
        return PLACE[(0, j) if half == 0 else (j, 0)], slice(first, first + 128), slice(None)

    def second_copy(half, w, stage):
        target = (near2.at[half, w], far2.at[half, w, 1], far2.at[half, w, 0])[stage]
        place, rows, _ = home_at(half, (2, 1 + 2 * w, 1 + 2 * w)[stage], (w, 1 - w, w)[stage])
        return remote(p_ref.at[place, rows, :], target, send2.at[half, w, stage], recv2.at[half, w, stage],
                      device(1 - half, 1 - 2 * w))

    def arrive(half, j, part):
        far_copy(half, part, 2, j).wait_recv()
        far_copy(half, 1 - part, 1, j).wait_recv()

    def total(half, j, part):
        value = p_ref[home_at(half, j, part)].astype(f32) + mail[4 + (half * 2 + part) * 2, j].astype(f32)
        return value + mail[4 + (half * 2 + 1 - part) * 2 + 1, j].astype(f32)

    def home(half, j):
        for part in range(2):
            if j == 2 or part == 1 - (j - 1) // 2:
                arrive(half, j, part)
                p_ref[home_at(half, j, part)] = total(half, j, part).astype(jnp.bfloat16)
                if j == 2:
                    second_copy(half, part, 0).start()
                else:
                    second_copy(half, 1 - part, 1).start()

    def after(c):
        send_place(c)
        for (half, w, j), at in CARRY_AT.items():
            if at == c:
                carry(half, w, j)
        for (half, j), at in HOME_AT.items():
            if at == c:
                home(half, j)
        if c == RELAY_AT:
            for copy in spread:
                copy.wait_recv()
            for copy in relay:
                copy.start()
        if c == HAND_AT:
            for copy in relay:
                copy.wait_recv()
            for copy in hand:
                copy.start()

    step(ORDER[0][0], ORDER[0][1], gb0, c0, rc0)

    def two(i, codes):
        cx, cy = codes
        p_ref[2 * i] = multiply(gb0, c0, rc0)
        for place in range(7):
            @pl.when(i == place)
            def _():
                after(2 * place)
        step(lax.rem(cx, 4), lax.rem(cy, 4), gb1, c1, rc1)
        cx, cy = cx // 4, cy // 4
        p_ref[2 * i + 1] = multiply(gb1, c1, rc1)
        for place in range(7):
            @pl.when(i == place)
            def _():
                after(2 * place + 1)
        step(lax.rem(cx, 4), lax.rem(cy, 4), gb0, c0, rc0)
        return cx // 4, cy // 4
    lax.fori_loop(0, 7, two, (jnp.int32(CODE[0] // 4), jnp.int32(CODE[1] // 4)))
    p_ref[14] = multiply(gb0, c0, rc0)
    after(14)
    step(ORDER[15][0], ORDER[15][1], gb1, c1, rc1)
    p_ref[15] = multiply(gb1, c1, rc1)
    after(15)

    own_copy.wait()
    for copy in hand:
        copy.wait_recv()

    def load(i, slot):
        block = lax.rem(q + i + 1, 8)
        return pltpu.make_async_copy(all_ref.at[pl.ds(block * 2, 2)], mail.at[pl.ds(slot * 2, 2)], load_sem.at[slot])

    load(0, 0).start()
    load(1, 1).start()

    for half in range(2):
        for w in range(2):
            second_copy(half, w, 0).wait_recv()
            arrive(half, 1 + 2 * w, w)
            value = total(half, 1 + 2 * w, w) + near2[half, w].astype(f32)
            p_ref[home_at(half, 1 + 2 * w, w)] = value.astype(jnp.bfloat16)
            second_copy(half, w, 2).start()
    for half in range(2):
        for w in range(2):
            second_copy(half, w, 1).wait_recv()
            second_copy(half, w, 2).wait_recv()
        for w in range(2):
            rows = slice(256 * half + 128 * w, 256 * half + 128 * w + 128)
            arrive(half, 0, w)
            value = total(half, 0, w) + far2[half, w, 0].astype(f32) + far2[half, 1 - w, 1].astype(f32)
            hidden = jnp.maximum(value + bias_ref[...], 0.0)
            inv = lax.rsqrt(jnp.mean(hidden * hidden, axis=-1, keepdims=True) + 0.25)
            embed = (hidden * inv).astype(jnp.bfloat16)
            embed_ref[rows, :] = embed
            c0[rows, 0:512] = embed * jnp.bfloat16(0.25)
    for i in range(2, 6):
        load(i, i).start()

    def block_copy(d):
        return remote(stats.at[d - 1], got.at[q], send3.at[d - 1], recv3.at[d - 1], row_peers[d - 1])

    def block(i, _):
        slot = lax.rem(i, 6)
        load(i, slot).wait()
        for part in range(2):
            cols = pl.ds(part * 512, 512)
            scores = lax.dot_general(
                c0[:, 0:512], mail[2 * slot + part].reshape(512, 512), (((1,), (1,)), ((), ())),
                preferred_element_type=f32)
            scores = scores - jnp.concatenate([logc_ref[...]] * 4, axis=1)
            peak = jnp.max(scores, axis=0, keepdims=True)
            total = jnp.sum(jnp.exp(scores - peak), axis=0, keepdims=True)
            stats[i, 0:1, cols] = peak
            stats[i, 1:2, cols] = total
        for d in range(1, 8):
            @pl.when(i == d - 1)
            def _():
                block_copy(d).start()

        @pl.when(i < 2)
        def _():
            load(i + 6, slot).start()
        return 0
    lax.fori_loop(0, 8, block, 0)
    got[q] = stats[7]
    last_copies = [block_copy(d) for d in range(1, 8)]
    for copy in last_copies:
        copy.wait_recv()
    peak, total = joined(got[...])
    mine[...] = jnp.concatenate([peak, total], axis=0)
    final[me] = mine[...]
    for d, peer in enumerate(peers):
        last_copies.append(remote(mine, final.at[me], send4.at[d], recv4.at[d], peer))
        last_copies[-1].start()
    for copy in last_copies[7:]:
        copy.wait_recv()
    peak, total = joined(final[...])
    lse_ref[...] = peak + jnp.log(total) - math.log(65536)

    for copy in row_copies + aux_copies + spread + relay + hand + last_copies:
        copy.wait_send()
    for half in range(2):
        for w in range(2):
            for j in range(4):
                near_copy(half, w, j).wait_send()
                far_copy(half, w, 1, j).wait_send()
                far_copy(half, w, 2, j).wait_send()
            for stage in range(3):
                second_copy(half, w, stage).wait_send()


def joined(stats):
    peak = jnp.max(stats[:, 0:1, :], axis=0)
    total = jnp.sum(stats[:, 1:2, :] * jnp.exp(stats[:, 0:1, :] - peak[None]), axis=0)
    return peak, total


def tower(fetch_rows, slots, count, slot, table, wm, ws, wn, bm, bias, sampled, queries):
    any_space = pl.BlockSpec(memory_space=pl.ANY)
    bf16, f32, i32 = jnp.bfloat16, jnp.float32, jnp.int32
    dma = pltpu.SemaphoreType.DMA
    return pl.pallas_call(
        tower_kernel,
        out_shape=(
            jax.ShapeDtypeStruct((512, 512), bf16),
            jax.ShapeDtypeStruct((1, 1024), f32),
            jax.ShapeDtypeStruct((16, 4, 128, 512), bf16),
        ),
        in_specs=[VMEM] * 4 + [any_space] * 4 + [VMEM] * 3 + [any_space],
        out_specs=(VMEM, VMEM, any_space),
        scratch_shapes=[
            pltpu.VMEM((8192, 8, 128), f32),
            pltpu.VMEM((2, 512, 512), bf16),
            pltpu.VMEM((5768, 128), f32),
            pltpu.VMEM((640, 1024), bf16),
            pltpu.VMEM((640, 1024), bf16),
            pltpu.VMEM((512, 1280), bf16),
            pltpu.VMEM((512, 1280), bf16),
            pltpu.VMEM((512, 1), f32),
            pltpu.VMEM((512, 1), f32),
            pltpu.VMEM((48, 512), i32),
            pltpu.VMEM((48, 512), i32),
            pltpu.VMEM((512, 128), f32),
            pltpu.VMEM((512, 128), f32),
            pltpu.VMEM((16, 512, 512), bf16),
            pltpu.VMEM((512, 512), bf16),
            pltpu.VMEM((512, 512), bf16),
            pltpu.VMEM((512, 512), bf16),
            pltpu.VMEM((64, 128), i32),
            pltpu.VMEM((16, 1, 640), i32),
            pltpu.VMEM((16, 1, 640), i32),
            pltpu.SMEM((10240,), i32),
            pltpu.VMEM((24, 512), i32),
            pltpu.VMEM((16, 24, 512), i32),
            pltpu.VMEM((12, 4, 128, 512), bf16),
            pltpu.VMEM((2, 2, 128, 512), bf16),
            pltpu.VMEM((2, 2, 2, 128, 512), bf16),
            pltpu.VMEM((512, 128), f32),
            pltpu.VMEM((8, 2, 1024), f32),
            pltpu.VMEM((8, 2, 1024), f32),
            pltpu.VMEM((2, 1024), f32),
            pltpu.VMEM((16, 2, 1024), f32),
            dma((3,)), dma((4,)),
            dma((15,)), dma((15,)), dma((15,)), dma((15,)),
            dma((16,)), dma, dma((9,)), dma((9,)),
            dma((2, 2, 3, 4)), dma((2, 2, 3, 4)), dma((2, 2, 3)), dma((2, 2, 3)),
            dma((6,)), dma((7,)), dma((7,)), dma((15,)), dma((15,)),
        ],
        compiler_params=pltpu.CompilerParams(
            collective_id=1, has_side_effects=True, vmem_limit_bytes=67043328),
        name="tower",
    )(fetch_rows, slots, count, slot, table, wm, ws, wn, bm, bias, sampled, queries)


def per_device(
    items_table,
    fetch_rows,
    neighbour_slots,
    neighbour_count,
    self_slot,
    negative_count,
    message_weight,
    message_bias,
    self_weight,
    neighbour_weight,
    output_bias,
    queries,
):
    negative_embed, query_lse, _ = tower(
        fetch_rows, neighbour_slots.T, neighbour_count.reshape(1, 512), self_slot.reshape(1, 512), items_table,
        message_weight, self_weight, neighbour_weight, message_bias.reshape(1, 512), output_bias.reshape(1, 512),
        negative_count.reshape(1, 4096), queries.reshape(2, 4, 128, 512))
    return negative_embed, query_lse.reshape(1024)


def solution(mesh):
    in_specs = (
        P("neg", None),
        P(("neg", "qry"), None),
        P(("neg", "qry"), None),
        P(("neg", "qry")),
        P(("neg", "qry")),
        P("neg"),
        P(),
        P(),
        P(),
        P(),
        P(),
        P("qry", None),
    )
    out_specs = (P(("neg", "qry"), None), P("qry"))
    return jax.shard_map(
        per_device, mesh=mesh, in_specs=in_specs, out_specs=out_specs, check_vma=False
    )
```
